256 devices in a mesh: seq: 16 (over x, y_lo, core), exp: 16 (over y_hi, z).
Axes of the slice: x: 4, y: 4 (y_hi: 2, y_lo: 2; y = y_hi * 2 + y_lo), z: 8, core: 2. Of those that a mesh axis runs over, the one named last changes fastest.
Arguments:
- queries: bfloat16 [8, 4096, 2048], P(None, 'seq', 'exp'), may hold values from -5 to 5
- keys: bfloat16 [8, 4096, 2048], P(None, 'seq', 'exp'), may hold values from -5 to 5
- values: bfloat16 [8, 4096, 2048], P(None, 'seq', 'exp'), may hold values from -170 to 170
- seg_ids: int32 [8, 4096], replicated, may hold values from 0 to 3, as said below
- norm_gain: float32 [2048], replicated, may hold values from 0.25 to 1.75
- router_w: bfloat16 [512, 64], replicated, may hold values from -0.25 to 0.25
- expert_ids: int32 [4096, 8, 4, 2], P(('seq', 'exp')), may hold values from 0 to 63, all different within a row; in each aligned block of 512 rows (0 to 511, 512 to 1023, ..., all dimensions but the last counted through in order) at most 32 rows name the same one
- w_in: bfloat16 [64, 512, 1024], P('exp'), may hold values from -0.25 to 0.25
- w_out: bfloat16 [64, 1024, 512], P('exp'), may hold values from -0.1875 to 0.1875
Outputs:
- normed: bfloat16 [8, 4096, 2048], P(None, ('seq', 'exp'))
- expert_mix: bfloat16 [8, 4096, 2048], P(None, ('seq', 'exp'))
The draws below stay inside these ranges and needn't reach their ends.
Inputs may be any that keep to these rules, and one draw needn't show every extreme that they name: `seg_ids`: in each sequence the numbers start at 0, never fall, and rise by one at each of 3 document starts; every start lies at an even position after the middle of the sequence. `expert_ids`: the 2 experts of a sub-token differ. Among the rows of one device (its 16 positions, all sequences, all sub-tokens) no expert is named more than 32 times; in every draw some device names some expert exactly 32 times.
All inputs are finite; a program needn't handle non-finite values.
Results may differ from the reference program's by a relative error of at most 0.015.
Values may be sent and summed in bfloat16 or wider, within the bound.
A program may use at most 128 MiB of HBM per device.

```python
import math
import jax
import jax.numpy as jnp
import numpy as np
from jax import lax

HD = 128
HEADS = 16
HF = 2048
SUB = 512
SUBS = 4
EXPERTS = 64
FFH = 1024
TOPK = 2
CAP = 32
DOCS = 4
SEQS = 8
TOK_DEV = 16
SEQ_LEN = 4096
N_SEQ = 16


def drawn_pair(key):
    shape = (SEQS, SEQ_LEN, HF)
    first = jnp.clip(jax.random.normal(jax.random.fold_in(key, 101), shape, jnp.float32), -5.0, 5.0)
    second = jnp.clip(jax.random.normal(jax.random.fold_in(key, 102), shape, jnp.float32), -5.0, 5.0)
    return (first, second)


def draw_queries(key, part):
    return drawn_pair(key)[0].astype(jnp.bfloat16)


def draw_keys(key, part):
    return drawn_pair(key)[1].astype(jnp.bfloat16)


def draw_values(key, part):
    shape = (SEQS, SEQ_LEN, HF)
    head_of = (jnp.arange(HF) // HD).astype(jnp.float32)
    exponent = head_of / max(HEADS - 1, 1)
    base = jnp.clip(jax.random.normal(jax.random.fold_in(key, 201), shape, jnp.float32), -4.0, 4.0)
    drawn = base * (3.0 ** exponent)[None, None, :]
    return drawn.astype(jnp.bfloat16)


def draw_seg_ids(key, part):
    stacked_rows = []
    for sequence in range(SEQS):
        picked = jax.random.permutation(jax.random.fold_in(key, 31 + sequence), SEQ_LEN // 4 - 1)[:DOCS - 1]
        bounds = 2 * (picked.astype(jnp.int32) + SEQ_LEN // 4 + 1)
        positions = jnp.arange(SEQ_LEN, dtype=jnp.int32)
        stacked_rows.append(jnp.sum((positions[:, None] >= bounds[None, :]).astype(jnp.int32), axis=1))
    return jnp.stack(stacked_rows).astype(jnp.int32)


def level_of(key, extent, shards, least, largest):
    def one(axis_at, blocks):
        draws = jax.random.uniform(jax.random.fold_in(jax.random.fold_in(key, 6), axis_at), (blocks,), jnp.float32, least / len(shards), largest / len(shards))
        return jnp.repeat(jnp.exp(draws), extent[axis_at] // blocks).reshape((-1,) + (1,) * (len(extent) - axis_at - 1))

    level = one(*shards[0])
    for cut in shards[1:]:
        level = level * one(*cut)
    return level


def shared_out(stream_key, own, number, rows, amount, top, reach, lean):
    order = jax.random.permutation(stream_key, amount)
    heavy_load, usual = portions_of(amount, rows * top, reach, lean, True), portions_of(amount, rows * top, reach, lean, False)
    places = jnp.arange(amount)

    def named(lengths, offset_by):
        used = int((lengths > 0).sum())
        fixed = max(1, used // 4)
        passed = fixed + (places - fixed + offset_by * (used - fixed)) % max(1, amount - fixed)
        return jnp.zeros((amount,), jnp.int32).at[order[jnp.where(places < fixed, places, passed)]].set(jnp.asarray(lengths, jnp.int32))

    lengths = jnp.where(number % 4 == 0, named(heavy_load, number // 4), named(usual, number - number // 4 - 1))
    mixed = jax.random.permutation(jax.random.fold_in(own, 3), amount)
    source_of, receiver = mixed[0:amount // 2 * 2:2], mixed[1:amount // 2 * 2:2]
    margin = jnp.minimum(lengths[source_of] - 1, reach - lengths[receiver]) // 2
    margin = jnp.where((source_of == order[0]) | (receiver == order[0]) | (lengths[receiver] == 0), 0, jnp.maximum(margin, 0))
    passed = jax.random.randint(jax.random.fold_in(own, 4), (amount // 2,), 0, 1 << 20) % (margin + 1)
    lengths = lengths.at[source_of].add(-passed).at[receiver].add(passed)
    labels = jnp.searchsorted(jnp.cumsum(lengths), jnp.arange(rows * top), side="right").astype(jnp.int32)
    grid = labels.reshape(top, rows).T
    grid = grid[jax.random.permutation(jax.random.fold_in(own, 1), rows)]
    offset_by = jax.random.randint(jax.random.fold_in(own, 2), (rows, 1), 0, top)
    return jnp.take_along_axis(grid, (jnp.arange(top)[None, :] + offset_by) % top, axis=1)


def portions_of(amount, total, most, slope, full):
    weights = [(1 << 20) // math.isqrt(grade ** slope) + 1 for grade in range(1, amount + 1)]
    largest = most if full else min(most, max(-(-total // amount), total * weights[0] // sum(weights)))
    least = 1 if total - largest >= amount - 1 else 0
    given, rest = [largest] + [least] * (amount - 1), total - largest - least * (amount - 1)
    while rest > 0:
        candidates = [i for i in range(1, amount) if given[i] < largest] or [i for i in range(1, amount) if given[i] < most]
        mass, left = sum([weights[i] for i in candidates]), rest
        for i in candidates:
            more = min(most - given[i], max(1, left * weights[i] // mass), rest)
            given[i] = given[i] + more
            rest = rest - more
    return np.array(given)


def bell_draw(rng, shape, deviation, most, pieces=(), kind=jnp.bfloat16):
    values = deviation * jax.random.normal(rng, shape, jnp.float32)
    if pieces:
        values = values * level_of(rng, shape, pieces, -0.22, 0.18)
    return jnp.clip(values, -most, most).astype(kind)


def setup_inputs(seed: int = 0) -> dict:
    key_list = jax.random.split(jax.random.key(seed), 10)
    queries = draw_queries(jax.random.fold_in(key_list[9], 71), 0)
    keys = draw_keys(jax.random.fold_in(key_list[9], 71), 0)
    values = draw_values(jax.random.fold_in(key_list[9], 71), 0)
    seg_ids = draw_seg_ids(jax.random.fold_in(key_list[9], 71), 0)
    norm_gain = jnp.clip(1.0 + 0.15 * jax.random.normal(key_list[4], (HF,), jnp.float32), 0.25, 1.75)
    router_w = bell_draw(key_list[5], (SUB, EXPERTS), SUB ** -0.5, 0.25)
    expert_ids_keys = jax.random.split(jax.random.fold_in(key_list[6], 1), SEQ_LEN * SEQS * SUBS // (TOK_DEV * SEQS * SUBS))
    expert_ids_turns = jax.random.permutation(jax.random.fold_in(key_list[6], 3), SEQ_LEN * SEQS * SUBS // (TOK_DEV * SEQS * SUBS))
    expert_ids = jax.vmap(lambda own, number: shared_out(jax.random.fold_in(key_list[6], 2), own, number, TOK_DEV * SEQS * SUBS, EXPERTS, TOPK, CAP, 2))(expert_ids_keys, expert_ids_turns).reshape((SEQ_LEN, SEQS, SUBS, TOPK))
    w_in = bell_draw(key_list[7], (EXPERTS, SUB, FFH), SUB ** -0.5, 0.25, ((0, 16),))
    w_out = bell_draw(key_list[8], (EXPERTS, FFH, SUB), FFH ** -0.5, 0.1875, ((0, 16),))
    return dict(queries=queries, keys=keys, values=values, seg_ids=seg_ids, norm_gain=norm_gain, router_w=router_w, expert_ids=expert_ids, w_in=w_in, w_out=w_out)


NEG = -1e+30

def update(running, query_slice, key_slice, value_slice, query_pos, query_seg, key_pos, key_seg, score_scale):
    maxima, totals, running_total = running
    attention_scores = jnp.einsum('uio,umo->uim', query_slice.astype(jnp.float32), key_slice.astype(jnp.float32)) * score_scale
    visible = (key_pos[None, :] <= query_pos[:, None])[None] & (key_seg[:, None, :] == query_seg[:, :, None])
    highest = lax.optimization_barrier(jnp.max(jnp.where(visible, attention_scores, NEG), axis=-1))
    new_max = jnp.maximum(maxima, highest)
    weights = jnp.where(visible, jnp.exp(attention_scores - new_max[..., None]), 0.0)
    rescale_factor = jnp.exp(maxima - new_max)
    totals = totals * rescale_factor + lax.optimization_barrier(jnp.sum(weights, axis=-1))
    rounded_result = weights.astype(jnp.bfloat16)
    running_total = running_total * rescale_factor[..., None] + jnp.einsum('uie,uec->uic', rounded_result.astype(jnp.float32), value_slice.astype(jnp.float32))
    return (new_max, totals, running_total)

def reference(queries, keys, values, seg_ids, norm_gain, router_w, expert_ids, w_in, w_out):
    local_len = SEQ_LEN // N_SEQ
    score_scale = HD ** (-0.5)

    def one_head(head):
        head_queries = lax.dynamic_slice_in_dim(queries, head * HD, HD, 2)
        head_keys = lax.dynamic_slice_in_dim(keys, head * HD, HD, 2)
        head_values = lax.dynamic_slice_in_dim(values, head * HD, HD, 2)

        def one_block(block_index):
            query_first = block_index * local_len
            query_slice = lax.dynamic_slice_in_dim(head_queries, query_first, local_len, 1)
            query_pos = query_first + jnp.arange(local_len, dtype=jnp.int32)
            query_seg = lax.dynamic_slice_in_dim(seg_ids, query_first, local_len, 1)
            initial = (jnp.full((SEQS, local_len), NEG, jnp.float32), jnp.zeros((SEQS, local_len), jnp.float32), jnp.zeros((SEQS, local_len, HD), jnp.float32))

            def over_keys(running, key_index):
                key_first = key_index * local_len
                key_slice = lax.dynamic_slice_in_dim(head_keys, key_first, local_len, 1)
                value_slice = lax.dynamic_slice_in_dim(head_values, key_first, local_len, 1)
                key_seg = lax.dynamic_slice_in_dim(seg_ids, key_first, local_len, 1)
                key_pos = key_first + jnp.arange(local_len, dtype=jnp.int32)
                needed = (key_first <= query_first + local_len - 1) & jnp.any(key_seg[:, -1] >= query_seg[:, 0])
                running = lax.cond(needed, lambda state: update(state, query_slice, key_slice, value_slice, query_pos, query_seg, key_pos, key_seg, score_scale), lambda state: state, running)
                return (running, None)
            final, unused = lax.scan(over_keys, initial, jnp.arange(N_SEQ, dtype=jnp.int32))
            return (final[2] / final[1][..., None]).astype(jnp.bfloat16)
        blocks = lax.map(one_block, jnp.arange(N_SEQ, dtype=jnp.int32))
        return blocks.transpose(1, 0, 2, 3).reshape(SEQS, SEQ_LEN, HD)
    heads = lax.map(one_head, jnp.arange(HEADS, dtype=jnp.int32))
    attended = heads.transpose(1, 2, 0, 3).reshape(SEQS, SEQ_LEN, HF)
    values32 = attended.astype(jnp.float32)
    spread = jnp.sqrt(lax.optimization_barrier(jnp.mean(values32 * values32, axis=-1, keepdims=True)) + 1e-06)
    normed = (values32 / spread * norm_gain).astype(jnp.bfloat16)
    sub_rows = normed.reshape(SEQS, SEQ_LEN, SUBS, SUB).transpose(1, 0, 2, 3).reshape(-1, SUB)
    picks = expert_ids.reshape(-1, TOPK)
    logits = jnp.dot(sub_rows, router_w, preferred_element_type=jnp.float32)
    chosen = jnp.take_along_axis(logits, picks, axis=1)
    sigmas = jax.nn.sigmoid(chosen)
    gates = sigmas / lax.optimization_barrier(jnp.sum(sigmas, axis=1, keepdims=True))
    targets = picks.reshape(-1).astype(jnp.int32)
    assign_count = targets.shape[0]
    order = jnp.argsort(targets, stable=True).astype(jnp.int32)
    counts = jax.ops.segment_sum(jnp.ones_like(targets), targets, num_segments=EXPERTS).astype(jnp.int32)
    block_rows = 512
    padded = ((counts + block_rows - 1) // block_rows * block_rows).astype(jnp.int32)
    padded_start = (jnp.cumsum(padded) - padded).astype(jnp.int32)
    plain_start = (jnp.cumsum(counts) - counts).astype(jnp.int32)
    sorted_targets = targets[order]
    within = jnp.arange(assign_count, dtype=jnp.int32) - plain_start[sorted_targets]
    placed = (padded_start[sorted_targets] + within).astype(jnp.int32)
    block_total = assign_count // block_rows + EXPERTS + 1
    owner = jnp.full((block_total * block_rows,), assign_count, jnp.int32).at[placed].set(order)
    padded_end = padded_start + padded
    block_first = jnp.arange(block_total, dtype=jnp.int32) * block_rows
    block_expert = jnp.minimum(lax.optimization_barrier(jnp.sum((padded_end[None, :] <= block_first[:, None]).astype(jnp.int32), axis=1)), EXPERTS - 1).astype(jnp.int32)

    def run_block(index):
        members = lax.dynamic_slice_in_dim(owner, index * block_rows, block_rows)
        inputs = sub_rows[jnp.minimum(members, assign_count - 1) // TOPK]
        expert = block_expert[index]
        hidden = jax.nn.gelu(jnp.dot(inputs, w_in[expert], preferred_element_type=jnp.float32), approximate=True).astype(jnp.bfloat16)
        return jnp.dot(hidden, w_out[expert], preferred_element_type=jnp.float32).astype(jnp.bfloat16)
    outputs = lax.map(run_block, jnp.arange(block_total, dtype=jnp.int32)).reshape(-1, SUB)
    per_assign = jnp.zeros((assign_count, SUB), jnp.bfloat16).at[owner].set(outputs, mode='drop')
    picked = per_assign.reshape(-1, TOPK, SUB).astype(jnp.float32)
    mixed = lax.optimization_barrier(jnp.sum(gates[:, :, None] * picked, axis=1)).astype(jnp.bfloat16)
    expert_mix = mixed.reshape(SEQ_LEN, SEQS, HF).transpose(1, 0, 2)
    return (normed, expert_mix)
```

```python
import functools

import jax
import jax.numpy as jnp
from jax import lax
from jax.experimental import pallas as pl
from jax.experimental.pallas import tpu as pltpu
from jax.sharding import PartitionSpec as P

HD = 128
SUB = 512
CAP = 32
NEG = -1e30
LOG2E = 1.4426950408889634

NS = 16
NE = 16
SEQS = 8
BLK = 256
HALF = 128
EPD = 4
ROWS = EPD * CAP
FFH = 1024
TOK = 16


def other(seq, exp):
    return {"seq": seq, "exp": exp}


def spread_kernel(q_ref, k_ref, v_ref, qo, ko, vo, loc, ksend, vsend, qsend, krecv, vrecv, qrecv, kfwd, vfwd):
    s = lax.axis_index("seq")
    e = lax.axis_index("exp")
    c = s // 2
    k = s % 2
    partner = 2 * c + 1 - k

    barrier = pltpu.get_barrier_semaphore()

    def greet(i, _):
        pl.semaphore_signal(barrier, inc=1, device_id=other((s + i) % NS, e), device_id_type=pl.DeviceIdType.MESH)
        return 0

    lax.fori_loop(1, NS, greet, 0)
    pl.semaphore_wait(barrier, NS - 1)

    def remote(src, dst, ss, rs, seq):
        return pltpu.make_async_remote_copy(
            src_ref=src, dst_ref=dst, send_sem=ss, recv_sem=rs,
            device_id=other(seq, e), device_id_type=pl.DeviceIdType.MESH,
        )

    def sends(j):
        b = (c + j) % SEQS
        same = 2 * b + k
        cross = 2 * b + 1 - k
        return (
            remote(k_ref.at[b], ko.at[s], ksend.at[j], krecv.at[s], same),
            remote(v_ref.at[b], vo.at[s], vsend.at[j], vrecv.at[s], same),
            remote(q_ref.at[b, k], qo.at[s], qsend.at[j], qrecv.at[s], same),
            remote(q_ref.at[b, 1 - k], qo.at[s], qsend.at[SEQS + j], qrecv.at[s], cross),
        )

    def start(j, _):
        for copy in sends(j):
            copy.start()
        return 0

    lax.fori_loop(1, SEQS, start, 0)

    own = (
        pltpu.make_async_copy(k_ref.at[c], ko.at[s], loc.at[0]),
        pltpu.make_async_copy(v_ref.at[c], vo.at[s], loc.at[1]),
        pltpu.make_async_copy(q_ref.at[c, k], qo.at[s], loc.at[2]),
    )
    near = (
        remote(k_ref.at[c], ko.at[s], kfwd.at[0], krecv.at[s], partner),
        remote(v_ref.at[c], vo.at[s], vfwd.at[0], vrecv.at[s], partner),
        remote(q_ref.at[c, 1 - k], qo.at[s], qsend.at[0], qrecv.at[s], partner),
    )
    for copy in own + near:
        copy.start()

    def forward(j):
        src = 2 * ((c + SEQS - j) % SEQS) + k
        return (
            remote(ko.at[src], ko.at[src], kfwd.at[j], krecv.at[src], partner),
            remote(vo.at[src], vo.at[src], vfwd.at[j], vrecv.at[src], partner),
        )

    def relay(j, _):
        for copy in forward(j):
            copy.wait_recv()
            copy.start()
        return 0

    lax.fori_loop(1, SEQS, relay, 0)

    def finish(j, _):
        src = 2 * ((c + SEQS - j) % SEQS) + 1 - k
        remote(ko.at[src], ko.at[src], kfwd.at[j], krecv.at[src], partner).wait_recv()
        remote(vo.at[src], vo.at[src], vfwd.at[j], vrecv.at[src], partner).wait_recv()
        return 0

    lax.fori_loop(0, SEQS, finish, 0)

    def finish_q(i, _):
        src = (s + i) % NS
        remote(qo.at[src], qo.at[src], qsend.at[0], qrecv.at[src], partner).wait_recv()
        return 0

    lax.fori_loop(1, NS, finish_q, 0)

    def drain(j, _):
        for copy in sends(j) + forward(j):
            copy.wait_send()
        return 0

    lax.fori_loop(1, SEQS, drain, 0)
    for copy in own:
        copy.wait()
    for copy in near:
        copy.wait_send()


def spread(queries, keys, values):
    hbm = pl.BlockSpec(memory_space=pl.ANY)
    dma = pltpu.SemaphoreType.DMA
    return pl.pallas_call(
        spread_kernel,
        out_shape=(
            jax.ShapeDtypeStruct((NS, HALF, HD), jnp.bfloat16),
            jax.ShapeDtypeStruct((NS, BLK, HD), jnp.bfloat16),
            jax.ShapeDtypeStruct((NS, BLK, HD), jnp.bfloat16),
        ),
        in_specs=[hbm] * 3,
        out_specs=(hbm, hbm, hbm),
        scratch_shapes=[
            dma((3,)), dma((SEQS,)), dma((SEQS,)), dma((2 * SEQS,)),
            dma((NS,)), dma((NS,)), dma((NS,)), dma((SEQS,)), dma((SEQS,)),
        ],
        compiler_params=pltpu.CompilerParams(collective_id=0, has_side_effects=True),
        name="spread",
    )(queries.reshape(SEQS, 2, HALF, HD), keys, values)


QG = 256
KC = 512
GROUPS = 8


def attention_kernel(seg_ref, q_ref, k_ref, v_ref, o_ref, mx_ref, sum_ref, acc_ref):
    s = lax.axis_index("seq")
    c = s // 2
    k = s % 2
    seg = seg_ref[pl.ds(c, 1), :]
    firsts = [jnp.sum((seg < v).astype(jnp.int32)) for v in (1, 2, 3)]
    scale = HD ** (-0.5) * LOG2E

    for m in range(GROUPS):
        first_pos = m * KC + k * HALF
        lowest = 0
        for f in firsts:
            lowest = jnp.where(f <= first_pos, f, lowest)
        mx_ref[...] = jnp.full((QG, HD), NEG, jnp.float32)
        sum_ref[...] = jnp.zeros((QG, HD), jnp.float32)
        acc_ref[...] = jnp.zeros((QG, HD), jnp.float32)

        def chunk(j, _):
            kk = k_ref[pl.ds(2 * j, 2)].reshape(KC, HD)
            vv = v_ref[pl.ds(2 * j, 2)].reshape(KC, HD)
            base = j * KC
            for half in range(2):
                rows = pl.ds(half * HALF, HALF)
                qq = q_ref[2 * m + half]
                scores = lax.dot_general(qq, kk, (((1,), (1,)), ((), ())), preferred_element_type=jnp.float32)
                pos = lax.broadcasted_iota(jnp.int32, (HALF, 1), 0) + (first_pos + half * BLK)
                begin = jnp.zeros((HALF, 1), jnp.int32)
                for f in firsts:
                    begin = jnp.where(pos >= f, f, begin)
                key_pos = lax.broadcasted_iota(jnp.int32, (HALF, KC), 1)
                scores = jnp.where((key_pos <= pos - base) & (key_pos >= begin - base), scores, NEG)
                old = mx_ref[rows, 0:1]
                new = jnp.maximum(old, jnp.max(scores, axis=-1, keepdims=True))
                weights = jnp.exp2((scores - new) * scale)
                factor = jnp.exp2((old - new) * scale)
                part = weights[:, 0:HD]
                for i in range(1, KC // HD):
                    part = part + weights[:, i * HD:(i + 1) * HD]
                sum_ref[rows, :] = sum_ref[rows, :] * factor + part
                acc_ref[rows, :] = acc_ref[rows, :] * factor + jnp.dot(
                    weights.astype(jnp.bfloat16), vv, preferred_element_type=jnp.float32
                )
                mx_ref[rows, :] = jnp.broadcast_to(new, (HALF, HD))
            return 0

        lax.fori_loop(lowest // KC, m + 1, chunk, 0)
        total = jnp.sum(sum_ref[...], axis=-1, keepdims=True)
        o_ref[2 * m:2 * m + 2] = (acc_ref[...] / total).astype(jnp.bfloat16).reshape(2, HALF, HD)


def attention(seg_ids, q, k, v):
    vmem = pl.BlockSpec(memory_space=pltpu.VMEM)
    return pl.pallas_call(
        attention_kernel,
        out_shape=jax.ShapeDtypeStruct((NS, HALF, HD), jnp.bfloat16),
        in_specs=[vmem] * 4,
        out_specs=vmem,
        scratch_shapes=[pltpu.VMEM((QG, HD), jnp.float32)] * 3,
        name="attention",
    )(seg_ids, q, k, v)


def moe_kernel(
    o_ref, ids_ref, gain_ref, rw_ref, win_hbm, wout_hbm, normed_ref, mix_ref,
    tok, xbuf, outbuf, arrived, res, returned, win, wout, acc, cols, spare,
    wsem, osend, orecv, dsend, drecv, rsend, rrecv,
):
    s = lax.axis_index("seq")
    e = lax.axis_index("exp")
    c = s // 2
    k = s % 2
    f32, bf16 = jnp.float32, jnp.bfloat16
    mesh_id = pl.DeviceIdType.MESH

    loads = (
        pltpu.make_async_copy(win_hbm, win, wsem.at[0]),
        pltpu.make_async_copy(wout_hbm, wout, wsem.at[1]),
    )
    for copy in loads:
        copy.start()

    barrier = pltpu.get_barrier_semaphore()
    number = s * NE + e

    def greet(i, _):
        t = (number + i) % (NS * NE)
        pl.semaphore_signal(barrier, inc=1, device_id=other(t // NE, t % NE), device_id_type=mesh_id)
        return 0

    lax.fori_loop(1, NS * NE, greet, 0)
    pl.semaphore_wait(barrier, NS * NE - 1)

    def give(i, _):
        sp = (s + i // 8) % NS
        ei = (e + i) % 8
        ep = k * 8 + ei
        mine = (sp == s) & (ep == e)

        @pl.when(jnp.logical_not(mine))
        def _():
            pltpu.make_async_remote_copy(
                src_ref=o_ref.at[sp, ei], dst_ref=tok.at[c, e], send_sem=osend, recv_sem=orecv.at[c],
                device_id=other(sp, ep), device_id_type=mesh_id,
            ).start()

        @pl.when(mine)
        def _():
            pltpu.make_async_copy(o_ref.at[sp, ei], tok.at[c, e], orecv.at[c]).start()
            pltpu.make_async_copy(o_ref.at[sp, ei], spare, osend).start()

        return 0

    lax.fori_loop(0, 8 * NS, give, 0)

    ids = ids_ref[...]
    experts = lax.broadcasted_iota(jnp.int32, (64, SUB), 0)
    before = (
        lax.broadcasted_iota(jnp.int32, (SUB, SUB), 0) < lax.broadcasted_iota(jnp.int32, (SUB, SUB), 1)
    ).astype(f32).astype(bf16)
    hot0 = (experts == ids[0:1]).astype(f32)
    hot1 = (experts == ids[1:2]).astype(f32)
    run0 = jnp.dot(hot0.astype(bf16), before, preferred_element_type=f32)
    run1 = jnp.dot(hot1.astype(bf16), before, preferred_element_type=f32)
    run1 = run1 + jnp.sum(hot0, axis=1, keepdims=True)
    idf = ids.astype(f32)
    slot0 = idf[0:1] * CAP + jnp.sum(run0 * hot0, axis=0, keepdims=True)
    slot1 = idf[1:2] * CAP + jnp.sum(run1 * hot1, axis=0, keepdims=True)
    lines = jnp.concatenate([slot0, slot1, idf, jnp.zeros((124, SUB), f32)], axis=0)
    lines = jnp.transpose(lines)
    cols[0] = jnp.broadcast_to(lines[:, 0:1], (SUB, HD))
    cols[1] = jnp.broadcast_to(lines[:, 1:2], (SUB, HD))
    lanes64 = lax.broadcasted_iota(jnp.int32, (SUB, 64), 1).astype(f32)
    pick0 = lanes64 == lines[:, 2:3]
    pick1 = lanes64 == lines[:, 3:4]

    gain = gain_ref[...]

    def norm(b, _):
        pltpu.make_async_copy(tok.at[b], tok.at[b], orecv.at[b]).wait()
        v = tok[b].astype(f32)
        square = jnp.sum(jnp.sum(v * v, axis=0), axis=-1, keepdims=True)
        spread_ = jnp.sqrt(square * (1.0 / 2048.0) + 1e-6)
        n = (v / spread_[None] * gain[:, None, :]).astype(bf16)
        for h in range(16):
            normed_ref[b, :, h * HD:(h + 1) * HD] = n[h]
            xbuf[b * 4 + h // 4, :, (h % 4) * HD:(h % 4 + 1) * HD] = n[h]
        return 0

    lax.fori_loop(0, SEQS, norm, 0)

    x = xbuf[...].reshape(SUB, SUB)

    def sending(i):
        d = (e + i) % NE
        return pltpu.make_async_remote_copy(
            src_ref=outbuf.at[i], dst_ref=arrived.at[e], send_sem=dsend.at[i], recv_sem=drecv.at[e],
            device_id=other(s, d), device_id_type=mesh_id,
        )

    slot_line = lax.broadcasted_iota(jnp.int32, (ROWS, SUB), 0)

    def gathered(i):
        d = (e + i) % NE
        slot = (slot_line + d * ROWS).astype(f32)
        chosen = ((slot == slot0) | (slot == slot1)).astype(f32).astype(bf16)
        rows = jnp.dot(chosen, xbuf[...].reshape(SUB, SUB), preferred_element_type=f32)
        return rows.astype(bf16).reshape(EPD, CAP, SUB)

    def dispatch(i, _):
        outbuf[i] = gathered(i)
        sending(i).start()
        return 0

    lax.fori_loop(1, NE, dispatch, 0)
    arrived[e] = gathered(0)

    logits = jnp.dot(x, rw_ref[...], preferred_element_type=f32)
    sig0 = 1.0 / (1.0 + jnp.exp(-jnp.sum(jnp.where(pick0, logits, 0.0), axis=1, keepdims=True)))
    sig1 = 1.0 / (1.0 + jnp.exp(-jnp.sum(jnp.where(pick1, logits, 0.0), axis=1, keepdims=True)))
    cols[2] = jnp.broadcast_to(sig0 / (sig0 + sig1), (SUB, HD))
    cols[3] = jnp.broadcast_to(sig1 / (sig0 + sig1), (SUB, HD))
    acc[...] = jnp.zeros((SUB, SUB), f32)

    for copy in loads:
        copy.wait()

    def giving(i):
        src = (e + NE - i) % NE
        return pltpu.make_async_remote_copy(
            src_ref=res.at[i], dst_ref=returned.at[e], send_sem=rsend.at[i], recv_sem=rrecv.at[e],
            device_id=other(s, src), device_id_type=mesh_id,
        )

    def group(q, _):
        sources = [(e + NE - (q * 4 + j)) % NE for j in range(4)]
        for j in range(4):
            src = sources[j]

            @pl.when(src != e)
            def _():
                pltpu.make_async_copy(arrived.at[src], arrived.at[src], drecv.at[src]).wait()

        def one(xp, _):
            a = jnp.concatenate([arrived[src, xp] for src in sources], axis=0)
            u = jnp.dot(a, win[xp], preferred_element_type=f32)
            hid = 0.5 * u * (1.0 + jnp.tanh(0.7978845608028654 * (u + 0.044715 * (u * u * u))))
            y = jnp.dot(hid.astype(bf16), wout[xp], preferred_element_type=f32).astype(bf16)
            for j in range(4):
                res[q * 4 + j, xp] = y[j * CAP:(j + 1) * CAP]
            return 0

        lax.fori_loop(0, EPD, one, 0)
        for j in range(4):
            i = q * 4 + j

            @pl.when(i != 0)
            def _():
                giving(i).start()

        return 0

    lax.fori_loop(0, 4, group, 0)
    returned[e] = res[0]

    lane = lax.broadcasted_iota(jnp.int32, (SUB, HD), 1)

    def combine(p, _):
        parts = []
        tables = []
        for j in range(2):
            d = (e + 2 * p + j) % NE

            @pl.when(d != e)
            def _():
                pltpu.make_async_copy(returned.at[d], returned.at[d], rrecv.at[d]).wait()

            slot = (lane + d * ROWS).astype(f32)
            tables.append(
                jnp.where(slot == cols[0], cols[2], 0.0) + jnp.where(slot == cols[1], cols[3], 0.0)
            )
            parts.append(returned[d].reshape(ROWS, SUB))
        table = jnp.concatenate(tables, axis=1)
        rows = jnp.concatenate(parts, axis=0)
        high = table.astype(bf16)
        low = (table - high.astype(f32)).astype(bf16)
        acc[...] += jnp.dot(high, rows, preferred_element_type=f32) + jnp.dot(low, rows, preferred_element_type=f32)
        return 0

    lax.fori_loop(0, NE // 2, combine, 0)
    for b in range(SEQS):
        for g in range(4):
            mix_ref[b, :, g * SUB:(g + 1) * SUB] = acc[(b * 4 + g) * TOK:(b * 4 + g + 1) * TOK].astype(bf16)

    pltpu.make_async_copy(o_ref, o_ref, osend).wait()

    def drain(i, _):
        sending(i).wait_send()
        giving(i).wait_send()
        return 0

    lax.fori_loop(1, NE, drain, 0)


def moe(o, ids, gain, router_w, w_in, w_out):
    vmem = pl.BlockSpec(memory_space=pltpu.VMEM)
    hbm = pl.BlockSpec(memory_space=pl.ANY)
    dma = pltpu.SemaphoreType.DMA
    bf16, f32 = jnp.bfloat16, jnp.float32
    return pl.pallas_call(
        moe_kernel,
        out_shape=(
            jax.ShapeDtypeStruct((SEQS, TOK, 2048), bf16),
            jax.ShapeDtypeStruct((SEQS, TOK, 2048), bf16),
        ),
        in_specs=[vmem] * 4 + [hbm] * 2,
        out_specs=(vmem, vmem),
        scratch_shapes=[
            pltpu.VMEM((SEQS, NE, TOK, HD), bf16),
            pltpu.VMEM((32, TOK, SUB), bf16),
            pltpu.VMEM((NE, EPD, CAP, SUB), bf16),
            pltpu.VMEM((NE, EPD, CAP, SUB), bf16),
            pltpu.VMEM((NE, EPD, CAP, SUB), bf16),
            pltpu.VMEM((NE, EPD, CAP, SUB), bf16),
            pltpu.VMEM((EPD, SUB, FFH), bf16),
            pltpu.VMEM((EPD, FFH, SUB), bf16),
            pltpu.VMEM((SUB, SUB), f32),
            pltpu.VMEM((4, SUB, HD), f32),
            pltpu.VMEM((TOK, HD), bf16),
            dma((2,)), dma(()), dma((SEQS,)), dma((NE,)), dma((NE,)), dma((NE,)), dma((NE,)),
        ],
        compiler_params=pltpu.CompilerParams(
            collective_id=1, has_side_effects=True, vmem_limit_bytes=56 * 1024 * 1024
        ),
        name="moe",
    )(o, ids, gain, router_w, w_in, w_out)


def body(queries, keys, values, seg_ids, norm_gain, router_w, expert_ids, w_in, w_out):
    q, k, v = spread(queries, keys, values)
    o = attention(seg_ids, q, k, v)
    ids = expert_ids.transpose(3, 1, 2, 0).reshape(2, SUB)
    return moe(
        o.reshape(NS, 8, TOK, HD), ids, norm_gain.reshape(16, HD), router_w, w_in, w_out
    )


def solution(mesh):
    return jax.shard_map(
        body,
        mesh=mesh,
        in_specs=(
            P(None, "seq", "exp"),
            P(None, "seq", "exp"),
            P(None, "seq", "exp"),
            P(),
            P(),
            P(),
            P(("seq", "exp"), None, None, None),
            P("exp", None, None),
            P("exp", None, None),
        ),
        out_specs=(P(None, ("seq", "exp"), None), P(None, ("seq", "exp"), None)),
        check_vma=False,
    )
```

```python
import functools

import jax
import jax.numpy as jnp
from jax import lax
from jax.experimental import pallas as pl
from jax.experimental.pallas import tpu as pltpu
from jax.sharding import PartitionSpec as P

HD = 128
SUB = 512
CAP = 32
NEG = -1e30
LOG2E = 1.4426950408889634

NS = 16
NE = 16
SEQS = 8
BLK = 256
HALF = 128
EPD = 4
ROWS = EPD * CAP
FFH = 1024
TOK = 16

QG = 256
KC = 512
GROUPS = 8
BIG = 2.0**100
MESH = pl.DeviceIdType.MESH


def other(seq, exp):
    return {"seq": seq, "exp": exp}


def offset_of(i):
    p = i // 2
    mag = 4 - (p + 1) // 2
    return (i + 1) % 2, jnp.where(p % 2 == 0, NZ - mag, mag)


NZ = 8


def partner_to(e, i):
    dy, dz = offset_of(i)
    return (e // NZ + dy) % 2 * NZ + (e % NZ + dz) % NZ


def partner_from(e, i):
    dy, dz = offset_of(i)
    return (e // NZ + dy) % 2 * NZ + (e % NZ + NZ - dz) % NZ


def kernel(
    q_ref, k_ref, v_ref, seg_ref, ids_ref, gain_ref, rw_ref, win_hbm, wout_hbm, normed_ref, mix_ref,
    qbuf, kbuf, vbuf, qaug, kaug, sbuf, pmax, mrow, asum, aacc, obuf,
    tok, xbuf, outbuf, arrived, res, returned, win, wout, acc, cols, spare,
    ready, loc, ksend, vsend, qsend, krecv, vrecv, qrecv, kfwd, vfwd,
    wsem, osend, orecv, dsend, drecv, rsend, rrecv,
):
    s = lax.axis_index("seq")
    e = lax.axis_index("exp")
    c = s // 2
    k = s % 2
    other_core = 2 * c + 1 - k
    f32, bf16 = jnp.float32, jnp.bfloat16

    loads = (
        pltpu.make_async_copy(win_hbm, win, wsem.at[0]),
        pltpu.make_async_copy(wout_hbm, wout, wsem.at[1]),
    )

    barrier = pltpu.get_barrier_semaphore()

    def greet(i, _):
        pl.semaphore_signal(barrier, inc=1, device_id=other((s + i) % NS, e), device_id_type=MESH)
        pl.semaphore_signal(barrier, inc=1, device_id=other(s, (e + i) % NE), device_id_type=MESH)
        return 0

    lax.fori_loop(1, NS, greet, 0)
    pl.semaphore_wait(barrier, 2 * (NS - 1))

    def remote(src, dst, ss, rs, seq, exp):
        return pltpu.make_async_remote_copy(
            src_ref=src, dst_ref=dst, send_sem=ss, recv_sem=rs, device_id=other(seq, exp), device_id_type=MESH
        )

    def sends(j):
        b = (c + j) % SEQS
        same = 2 * b + k
        cross = 2 * b + 1 - k
        return (
            remote(k_ref.at[b], kbuf.at[s], ksend.at[j], krecv.at[s], same, e),
            remote(v_ref.at[b], vbuf.at[s], vsend.at[j], vrecv.at[s], same, e),
            remote(q_ref.at[b, k], qbuf.at[s], qsend.at[j], qrecv.at[s], same, e),
            remote(q_ref.at[b, 1 - k], qbuf.at[s], qsend.at[SEQS + j], qrecv.at[s], cross, e),
        )

    def start(j, _):
        for copy in sends(j):
            copy.start()
        return 0

    lax.fori_loop(1, SEQS, start, 0)
    own = (
        pltpu.make_async_copy(k_ref.at[c], kbuf.at[s], loc.at[0]),
        pltpu.make_async_copy(v_ref.at[c], vbuf.at[s], loc.at[1]),
        pltpu.make_async_copy(q_ref.at[c, k], qbuf.at[s], loc.at[2]),
    )
    near = (
        remote(k_ref.at[c], kbuf.at[s], kfwd.at[0], krecv.at[s], other_core, e),
        remote(v_ref.at[c], vbuf.at[s], vfwd.at[0], vrecv.at[s], other_core, e),
        remote(q_ref.at[c, 1 - k], qbuf.at[s], qsend.at[0], qrecv.at[s], other_core, e),
    )
    for copy in own + near + loads:
        copy.start()

    def greet_again(i, _):
        pl.semaphore_signal(ready, inc=1, device_id=other(s, (e + i) % NE), device_id_type=MESH)
        return 0

    lax.fori_loop(1, NE, greet_again, 0)

    seg = seg_ref[pl.ds(c, 1), :]
    firsts = [jnp.sum((seg < v).astype(jnp.int32)) for v in (1, 2, 3)]

    def document(pos):
        return sum((pos >= f).astype(jnp.int32) for f in firsts)

    def mark(j, _):
        key_pos = lax.broadcasted_iota(jnp.int32, (KC, HD), 0) + j * KC
        lane = lax.broadcasted_iota(jnp.int32, (KC, HD), 1)
        kaug[j] = (document(key_pos) == lane).astype(f32).astype(bf16)
        row = lax.broadcasted_iota(jnp.int32, (QG, HD), 0)
        query_pos = row + jnp.where(row >= HALF, HALF, 0) + (j * KC + k * HALF)
        lane = lax.broadcasted_iota(jnp.int32, (QG, HD), 1)
        qaug[j] = jnp.where(document(query_pos) == lane, 0.0, -BIG).astype(bf16)
        return 0

    lax.fori_loop(0, GROUPS, mark, 0)

    ids = ids_ref[...]
    experts = lax.broadcasted_iota(jnp.int32, (64, SUB), 0)
    before = (
        lax.broadcasted_iota(jnp.int32, (SUB, SUB), 0) < lax.broadcasted_iota(jnp.int32, (SUB, SUB), 1)
    ).astype(f32).astype(bf16)
    hot0 = (experts == ids[0:1]).astype(f32)
    hot1 = (experts == ids[1:2]).astype(f32)
    run0 = jnp.dot(hot0.astype(bf16), before, preferred_element_type=f32)
    run1 = jnp.dot(hot1.astype(bf16), before, preferred_element_type=f32)
    run1 = run1 + jnp.sum(hot0, axis=1, keepdims=True)
    idf = ids.astype(f32)
    slot0 = idf[0:1] * CAP + jnp.sum(run0 * hot0, axis=0, keepdims=True)
    slot1 = idf[1:2] * CAP + jnp.sum(run1 * hot1, axis=0, keepdims=True)
    lines = jnp.concatenate([slot0, slot1, idf, jnp.zeros((124, SUB), f32)], axis=0)
    lines = jnp.transpose(lines)
    for i in range(4):
        cols[i] = jnp.broadcast_to(lines[:, i:i + 1], (SUB, HD))

    def forward(j):
        src = 2 * ((c + SEQS - j) % SEQS) + k
        return (
            remote(kbuf.at[src], kbuf.at[src], kfwd.at[j], krecv.at[src], other_core, e),
            remote(vbuf.at[src], vbuf.at[src], vfwd.at[j], vrecv.at[src], other_core, e),
        )

    def relay(j, _):
        for copy in forward(j):
            copy.wait_recv()
            copy.start()
        return 0

    lax.fori_loop(1, SEQS, relay, 0)

    def finish(j, _):
        src = 2 * ((c + SEQS - j) % SEQS) + 1 - k
        pltpu.make_async_copy(kbuf.at[src], kbuf.at[src], krecv.at[src]).wait()
        pltpu.make_async_copy(vbuf.at[src], vbuf.at[src], vrecv.at[src]).wait()
        return 0

    lax.fori_loop(0, SEQS, finish, 0)

    def finish_q(i, _):
        src = (s + i) % NS
        pltpu.make_async_copy(qbuf.at[src], qbuf.at[src], qrecv.at[src]).wait()
        return 0

    lax.fori_loop(1, NS, finish_q, 0)
    for copy in own:
        copy.wait()
    pl.semaphore_wait(ready, NE - 1)

    scale = HD ** (-0.5) * LOG2E

    def scores_of(m, j):
        qq = jnp.concatenate([qbuf[pl.ds(2 * m, 2)].reshape(QG, HD), qaug[m]], axis=1)
        kk = jnp.concatenate([kbuf[pl.ds(2 * j, 2)].reshape(KC, HD), kaug[j]], axis=1)
        return lax.dot_general(qq, kk, (((1,), (1,)), ((), ())), preferred_element_type=f32)

    def tiles(x, op):
        out = x[:, 0:HD]
        for i in range(1, KC // HD):
            out = op(out, x[:, i * HD:(i + 1) * HD])
        return out

    def first_pass(m, j):
        scores = scores_of(m, j)
        sbuf[m % 2, j] = scores
        pmax[m % 2] = jnp.maximum(pmax[m % 2], tiles(scores, jnp.maximum))

    def diagonal(m):
        scores = scores_of(m, m)
        row = lax.broadcasted_iota(jnp.int32, (QG, KC), 0)
        row = row + jnp.where(row >= HALF, HALF, 0) + k * HALF
        scores = jnp.where(lax.broadcasted_iota(jnp.int32, (QG, KC), 1) <= row, scores, -BIG)
        sbuf[m % 2, m] = scores
        highest = jnp.maximum(pmax[m % 2], tiles(scores, jnp.maximum))
        mrow[...] = jnp.broadcast_to(jnp.max(highest, axis=-1, keepdims=True), (QG, HD))

    def second_pass(m, j):
        top = mrow[...]
        top = jnp.concatenate([top] * (KC // HD), axis=1)
        weights = jnp.exp2((sbuf[m % 2, j] - top) * scale)
        asum[...] += tiles(weights, jnp.add)
        vv = vbuf[pl.ds(2 * j, 2)].reshape(KC, HD)
        aacc[...] += jnp.dot(weights.astype(bf16), vv, preferred_element_type=f32)

    def clear(m):
        pmax[m % 2] = jnp.full((QG, HD), -BIG, f32)

    def only_first(j, _):
        first_pass(c, j)
        return 0

    clear(c)
    lax.fori_loop(0, c, only_first, 0)
    diagonal(c)

    def attend(t, _):
        m = (c + t) % GROUPS
        after = (m + 1) % GROUPS
        asum[...] = jnp.zeros((QG, HD), f32)
        aacc[...] = jnp.zeros((QG, HD), f32)
        clear(after)
        both = (m < GROUPS - 1) & (t < GROUPS - 1)

        @pl.when(both)
        def _():
            def step(j, _):
                first_pass(m + 1, j)
                second_pass(m, j)
                return 0

            lax.fori_loop(0, m + 1, step, 0)

        @pl.when(jnp.logical_not(both))
        def _():
            def step(j, _):
                second_pass(m, j)
                return 0

            lax.fori_loop(0, m + 1, step, 0)

        total = jnp.sum(asum[...], axis=-1, keepdims=True)
        obuf[pl.ds(2 * m, 2)] = (aacc[...] / total).astype(bf16).reshape(2, 8, TOK, HD)

        def give(i, _):
            sp = 2 * m + i // 8
            ei = (e + i) % 8
            ep = k * 8 + ei
            mine = (sp == s) & (ep == e)

            @pl.when(jnp.logical_not(mine))
            def _():
                remote(obuf.at[sp, ei], tok.at[c, e], osend, orecv.at[c], sp, ep).start()

            @pl.when(mine)
            def _():
                pltpu.make_async_copy(obuf.at[sp, ei], tok.at[c, e], orecv.at[c]).start()
                pltpu.make_async_copy(obuf.at[sp, ei], spare, osend).start()

            return 0

        lax.fori_loop(0, 16, give, 0)

        @pl.when(t < GROUPS - 1)
        def _():
            diagonal(after)

        return 0

    lax.fori_loop(0, GROUPS, attend, 0)

    gain = gain_ref[...]

    def norm(b, _):
        pltpu.make_async_copy(tok.at[b], tok.at[b], orecv.at[b]).wait()
        v = tok[b].astype(f32)
        square = jnp.sum(jnp.sum(v * v, axis=0), axis=-1, keepdims=True)
        spread = jnp.sqrt(square * (1.0 / 2048.0) + 1e-6)
        n = (v / spread[None] * gain[:, None, :]).astype(bf16)
        for h in range(16):
            normed_ref[b, :, h * HD:(h + 1) * HD] = n[h]
            xbuf[b * 4 + h // 4, :, (h % 4) * HD:(h % 4 + 1) * HD] = n[h]
        return 0

    lax.fori_loop(0, SEQS, norm, 0)

    def sending(i):
        return remote(outbuf.at[i], arrived.at[e], dsend.at[i], drecv.at[e], s, partner_to(e, i))

    slot_line = lax.broadcasted_iota(jnp.int32, (ROWS, SUB), 0)

    def gathered(d):
        slot = (slot_line + d * ROWS).astype(f32)
        chosen = ((slot == slot0) | (slot == slot1)).astype(f32).astype(bf16)
        rows = jnp.dot(chosen, xbuf[...].reshape(SUB, SUB), preferred_element_type=f32)
        return rows.astype(bf16).reshape(EPD, CAP, SUB)

    def dispatch(i, _):
        outbuf[i] = gathered(partner_to(e, i))
        sending(i).start()
        return 0

    lax.fori_loop(0, NE - 1, dispatch, 0)
    arrived[e] = gathered(e)

    logits = jnp.dot(xbuf[...].reshape(SUB, SUB), rw_ref[...], preferred_element_type=f32)
    lanes64 = lax.broadcasted_iota(jnp.int32, (SUB, 64), 1).astype(f32)
    picked = [
        jnp.sum(jnp.where(lanes64 == cols[2 + t][:, 0:64], logits, 0.0), axis=1, keepdims=True) for t in range(2)
    ]
    sig0 = 1.0 / (1.0 + jnp.exp(-picked[0]))
    sig1 = 1.0 / (1.0 + jnp.exp(-picked[1]))
    cols[2] = jnp.broadcast_to(sig0 / (sig0 + sig1), (SUB, HD))
    cols[3] = jnp.broadcast_to(sig1 / (sig0 + sig1), (SUB, HD))
    acc[...] = jnp.zeros((SUB, SUB), f32)

    for copy in loads:
        copy.wait()

    def giving(i):
        return remote(res.at[i], returned.at[e], rsend.at[i], rrecv.at[e], s, partner_from(e, i))

    def group(q, _):
        sources = [partner_from(e, q * 4 + j) for j in range(4)]
        for j in range(4):
            src = sources[j]

            @pl.when(src != e)
            def _():
                pltpu.make_async_copy(arrived.at[src], arrived.at[src], drecv.at[src]).wait()

        def one(xp, _):
            a = jnp.concatenate([arrived[src, xp] for src in sources], axis=0)
            u = jnp.dot(a, win[xp], preferred_element_type=f32)
            hid = 0.5 * u * (1.0 + jnp.tanh(0.7978845608028654 * (u + 0.044715 * (u * u * u))))
            y = jnp.dot(hid.astype(bf16), wout[xp], preferred_element_type=f32).astype(bf16)
            for j in range(4):
                res[q * 4 + j, xp] = y[j * CAP:(j + 1) * CAP]
            return 0

        lax.fori_loop(0, EPD, one, 0)
        for j in range(4):
            i = q * 4 + j

            @pl.when(i != NE - 1)
            def _():
                giving(i).start()

        return 0

    lax.fori_loop(0, 4, group, 0)
    returned[e] = res[NE - 1]

    lane = lax.broadcasted_iota(jnp.int32, (SUB, HD), 1)

    def combine(p, _):
        parts = []
        tables = []
        for j in range(2):
            d = partner_to(e, 2 * p + j)

            @pl.when(d != e)
            def _():
                pltpu.make_async_copy(returned.at[d], returned.at[d], rrecv.at[d]).wait()

            slot = (lane + d * ROWS).astype(f32)
            tables.append(
                jnp.where(slot == cols[0], cols[2], 0.0) + jnp.where(slot == cols[1], cols[3], 0.0)
            )
            parts.append(returned[d].reshape(ROWS, SUB))
        table = jnp.concatenate(tables, axis=1)
        rows = jnp.concatenate(parts, axis=0)
        high = table.astype(bf16)
        low = (table - high.astype(f32)).astype(bf16)
        acc[...] += jnp.dot(high, rows, preferred_element_type=f32) + jnp.dot(low, rows, preferred_element_type=f32)
        return 0

    lax.fori_loop(0, NE // 2, combine, 0)
    for b in range(SEQS):
        for g in range(4):
            mix_ref[b, :, g * SUB:(g + 1) * SUB] = acc[(b * 4 + g) * TOK:(b * 4 + g + 1) * TOK].astype(bf16)

    pltpu.make_async_copy(obuf, obuf, osend).wait()

    def drain(j, _):
        for copy in sends(j) + forward(j):
            copy.wait_send()
        return 0

    lax.fori_loop(1, SEQS, drain, 0)
    for copy in near:
        copy.wait_send()

    def drain_rows(i, _):
        sending(i).wait_send()
        giving(i).wait_send()
        return 0

    lax.fori_loop(0, NE - 1, drain_rows, 0)


def body(queries, keys, values, seg_ids, norm_gain, router_w, expert_ids, w_in, w_out):
    ids = expert_ids.transpose(3, 1, 2, 0).reshape(2, SUB)
    vmem = pl.BlockSpec(memory_space=pltpu.VMEM)
    hbm = pl.BlockSpec(memory_space=pl.ANY)
    dma = pltpu.SemaphoreType.DMA
    bf16, f32 = jnp.bfloat16, jnp.float32
    return pl.pallas_call(
        kernel,
        out_shape=(
            jax.ShapeDtypeStruct((SEQS, TOK, 2048), bf16),
            jax.ShapeDtypeStruct((SEQS, TOK, 2048), bf16),
        ),
        in_specs=[hbm] * 3 + [vmem] * 4 + [hbm] * 2,
        out_specs=(vmem, vmem),
        scratch_shapes=[
            pltpu.VMEM((NS, HALF, HD), bf16),
            pltpu.VMEM((NS, BLK, HD), bf16),
            pltpu.VMEM((NS, BLK, HD), bf16),
            pltpu.VMEM((GROUPS, QG, HD), bf16),
            pltpu.VMEM((GROUPS, KC, HD), bf16),
            pltpu.VMEM((2, GROUPS, QG, KC), f32),
            pltpu.VMEM((2, QG, HD), f32),
            pltpu.VMEM((QG, HD), f32),
            pltpu.VMEM((QG, HD), f32),
            pltpu.VMEM((QG, HD), f32),
            pltpu.VMEM((NS, 8, TOK, HD), bf16),
            pltpu.VMEM((SEQS, NE, TOK, HD), bf16),
            pltpu.VMEM((32, TOK, SUB), bf16),
            pltpu.VMEM((NE, EPD, CAP, SUB), bf16),
            pltpu.VMEM((NE, EPD, CAP, SUB), bf16),
            pltpu.VMEM((NE, EPD, CAP, SUB), bf16),
            pltpu.VMEM((NE, EPD, CAP, SUB), bf16),
            pltpu.VMEM((EPD, SUB, FFH), bf16),
            pltpu.VMEM((EPD, FFH, SUB), bf16),
            pltpu.VMEM((SUB, SUB), f32),
            pltpu.VMEM((4, SUB, HD), f32),
            pltpu.VMEM((TOK, HD), bf16),
            pltpu.SemaphoreType.REGULAR,
            dma((3,)), dma((SEQS,)), dma((SEQS,)), dma((2 * SEQS,)),
            dma((NS,)), dma((NS,)), dma((NS,)), dma((SEQS,)), dma((SEQS,)),
            dma((2,)), dma(()), dma((SEQS,)), dma((NE,)), dma((NE,)), dma((NE,)), dma((NE,)),
        ],
        compiler_params=pltpu.CompilerParams(
            collective_id=0, has_side_effects=True, vmem_limit_bytes=56 * 1024 * 1024
        ),
        name="block",
    )(
        queries.reshape(SEQS, 2, HALF, HD), keys, values, seg_ids, ids,
        norm_gain.reshape(16, HD), router_w, w_in, w_out,
    )


def solution(mesh):
    return jax.shard_map(
        body,
        mesh=mesh,
        in_specs=(
            P(None, "seq", "exp"),
            P(None, "seq", "exp"),
            P(None, "seq", "exp"),
            P(),
            P(),
            P(),
            P(("seq", "exp"), None, None, None),
            P("exp", None, None),
            P("exp", None, None),
        ),
        out_specs=(P(None, ("seq", "exp"), None), P(None, ("seq", "exp"), None)),
        check_vma=False,
    )
```

```python
import functools

import jax
import jax.numpy as jnp
from jax import lax
from jax.experimental import pallas as pl
from jax.experimental.pallas import tpu as pltpu
from jax.sharding import PartitionSpec as P

HD = 128
SUB = 512
CAP = 32
NEG = -1e30
LOG2E = 1.4426950408889634

NS = 16
NE = 16
SEQS = 8
BLK = 256
HALF = 128
EPD = 4
ROWS = EPD * CAP
FFH = 1024
TOK = 16

QG = 256
KC = 512
GROUPS = 8
BIG = 2.0**100
MESH = pl.DeviceIdType.MESH


def other(seq, exp):
    return {"seq": seq, "exp": exp}


def offset_of(i):
    p = i // 2
    mag = 4 - (p + 1) // 2
    return (i + 1) % 2, jnp.where(p % 2 == 0, NZ - mag, mag)


NZ = 8


def partner_to(e, i):
    dy, dz = offset_of(i)
    return (e // NZ + dy) % 2 * NZ + (e % NZ + dz) % NZ


def partner_from(e, i):
    dy, dz = offset_of(i)
    return (e // NZ + dy) % 2 * NZ + (e % NZ + NZ - dz) % NZ


def kernel(
    q_ref, k_ref, v_ref, seg_ref, ids_ref, gain_ref, rw_ref, win_hbm, wout_hbm, normed_ref, mix_ref,
    qbuf, kbuf, vbuf, qaug, kaug, sbuf, pmax, mrow, asum, aacc, obuf,
    tok, xbuf, outbuf, arrived, res, returned, win, wout, acc, cols, spare,
    ready, loc, ksend, vsend, qsend, krecv, vrecv, qrecv, kfwd, vfwd,
    wsem, osend, orecv, dsend, drecv, rsend, rrecv,
):
    s = lax.axis_index("seq")
    e = lax.axis_index("exp")
    c = s // 2
    k = s % 2
    other_core = 2 * c + 1 - k
    f32, bf16 = jnp.float32, jnp.bfloat16

    loads = (
        pltpu.make_async_copy(win_hbm, win, wsem.at[0]),
        pltpu.make_async_copy(wout_hbm, wout, wsem.at[1]),
    )

    barrier = pltpu.get_barrier_semaphore()

    def greet(i, _):
        pl.semaphore_signal(barrier, inc=1, device_id=other((s + i) % NS, e), device_id_type=MESH)
        pl.semaphore_signal(barrier, inc=1, device_id=other(s, (e + i) % NE), device_id_type=MESH)
        return 0

    lax.fori_loop(1, NS, greet, 0)
    pl.semaphore_wait(barrier, 2 * (NS - 1))

    def remote(src, dst, ss, rs, seq, exp):
        return pltpu.make_async_remote_copy(
            src_ref=src, dst_ref=dst, send_sem=ss, recv_sem=rs, device_id=other(seq, exp), device_id_type=MESH
        )

    def send(which, j):
        b = (c + j) % SEQS
        same = 2 * b + k
        cross = 2 * b + 1 - k
        if which == 0:
            return remote(k_ref.at[b], kbuf.at[s], ksend.at[j], krecv.at[s], same, e)
        if which == 1:
            return remote(q_ref.at[b, k], qbuf.at[s], qsend.at[j], qrecv.at[s], same, e)
        if which == 2:
            return remote(q_ref.at[b, 1 - k], qbuf.at[s], qsend.at[SEQS + j], qrecv.at[s], cross, e)
        return remote(v_ref.at[b], vbuf.at[s], vsend.at[j], vrecv.at[s], same, e)

    def start_with(*which):
        def start(j, _):
            for i in which:
                send(i, j).start()
            return 0

        lax.fori_loop(1, SEQS, start, 0)

    start_with(0)
    own = (
        pltpu.make_async_copy(k_ref.at[c], kbuf.at[s], loc.at[0]),
        pltpu.make_async_copy(v_ref.at[c], vbuf.at[s], loc.at[1]),
        pltpu.make_async_copy(q_ref.at[c, k], qbuf.at[s], loc.at[2]),
    )
    near = (
        remote(k_ref.at[c], kbuf.at[s], kfwd.at[0], krecv.at[s], other_core, e),
        remote(v_ref.at[c], vbuf.at[s], vfwd.at[0], vrecv.at[s], other_core, e),
        remote(q_ref.at[c, 1 - k], qbuf.at[s], qsend.at[0], qrecv.at[s], other_core, e),
    )
    for copy in own + near:
        copy.start()
    start_with(3)
    start_with(1, 2)
    for copy in loads:
        copy.start()

    def greet_again(i, _):
        pl.semaphore_signal(ready, inc=1, device_id=other(s, (e + i) % NE), device_id_type=MESH)
        return 0

    lax.fori_loop(1, NE, greet_again, 0)

    seg = seg_ref[pl.ds(c, 1), :]
    firsts = [jnp.sum((seg < v).astype(jnp.int32)) for v in (1, 2, 3)]

    def document(pos):
        return sum((pos >= f).astype(jnp.int32) for f in firsts)

    def mark(j, _):
        key_pos = lax.broadcasted_iota(jnp.int32, (KC, HD), 0) + j * KC
        lane = lax.broadcasted_iota(jnp.int32, (KC, HD), 1)
        kaug[j] = (document(key_pos) == lane).astype(f32).astype(bf16)
        row = lax.broadcasted_iota(jnp.int32, (QG, HD), 0)
        query_pos = row + jnp.where(row >= HALF, HALF, 0) + (j * KC + k * HALF)
        lane = lax.broadcasted_iota(jnp.int32, (QG, HD), 1)
        qaug[j] = jnp.where(document(query_pos) == lane, 0.0, -BIG).astype(bf16)
        return 0

    lax.fori_loop(0, GROUPS, mark, 0)

    to_lane = (
        lax.broadcasted_iota(jnp.int32, (TOK, SUB), 0) == lax.broadcasted_iota(jnp.int32, (TOK, SUB), 1) % TOK
    ).astype(f32).astype(bf16)
    own_row = lax.broadcasted_iota(jnp.int32, (32, SUB), 0) == lax.broadcasted_iota(jnp.int32, (32, SUB), 1) // TOK
    ids = []
    for t in range(2):
        table = jnp.dot(ids_ref[:, t, :].astype(f32).astype(bf16), to_lane, preferred_element_type=f32)
        ids.append(jnp.sum(jnp.where(own_row, table, 0.0), axis=0, keepdims=True))
    experts = lax.broadcasted_iota(jnp.int32, (64, SUB), 0).astype(f32)
    before = (
        lax.broadcasted_iota(jnp.int32, (SUB, SUB), 0) < lax.broadcasted_iota(jnp.int32, (SUB, SUB), 1)
    ).astype(f32).astype(bf16)
    hot0 = (experts == ids[0]).astype(f32)
    hot1 = (experts == ids[1]).astype(f32)
    run0 = jnp.dot(hot0.astype(bf16), before, preferred_element_type=f32)
    run1 = jnp.dot(hot1.astype(bf16), before, preferred_element_type=f32)
    run1 = run1 + jnp.sum(hot0, axis=1, keepdims=True)
    slot0 = ids[0] * CAP + jnp.sum(run0 * hot0, axis=0, keepdims=True)
    slot1 = ids[1] * CAP + jnp.sum(run1 * hot1, axis=0, keepdims=True)
    lines = jnp.concatenate([slot0, slot1, *ids, jnp.zeros((124, SUB), f32)], axis=0)
    lines = jnp.transpose(lines)
    for i in range(4):
        cols[i] = jnp.broadcast_to(lines[:, i:i + 1], (SUB, HD))

    def forward(which, j):
        src = 2 * ((c + SEQS - j) % SEQS) + k
        if which == 0:
            return remote(kbuf.at[src], kbuf.at[src], kfwd.at[j], krecv.at[src], other_core, e)
        return remote(vbuf.at[src], vbuf.at[src], vfwd.at[j], vrecv.at[src], other_core, e)

    def relay_of(which):
        def relay(j, _):
            copy = forward(which, j)
            copy.wait_recv()
            copy.start()
            return 0

        lax.fori_loop(1, SEQS, relay, 0)

    def finish_of(buf, sem):
        def finish(j, _):
            src = 2 * ((c + SEQS - j) % SEQS) + 1 - k
            pltpu.make_async_copy(buf.at[src], buf.at[src], sem.at[src]).wait()
            return 0

        lax.fori_loop(0, SEQS, finish, 0)

    relay_of(0)
    relay_of(1)
    finish_of(kbuf, krecv)
    finish_of(vbuf, vrecv)
    for copy in own:
        copy.wait()
    pl.semaphore_wait(ready, NE - 1)

    scale = HD ** (-0.5) * LOG2E

    def scores_of(m, j):
        qq = jnp.concatenate([qbuf[pl.ds(2 * m, 2)].reshape(QG, HD), qaug[m]], axis=1)
        kk = jnp.concatenate([kbuf[pl.ds(2 * j, 2)].reshape(KC, HD), kaug[j]], axis=1)
        return lax.dot_general(qq, kk, (((1,), (1,)), ((), ())), preferred_element_type=f32)

    def tiles(x, op):
        out = x[:, 0:HD]
        for i in range(1, KC // HD):
            out = op(out, x[:, i * HD:(i + 1) * HD])
        return out

    def first_pass(m, j, count):
        highest = pmax[...]
        for i in range(count):
            scores = scores_of(m, j + i)
            sbuf[j + i] = scores
            highest = jnp.maximum(highest, tiles(scores, jnp.maximum))
        pmax[...] = highest

    def second_pass(m, j, count):
        top = jnp.concatenate([mrow[...]] * (KC // HD), axis=1)
        total = asum[...]
        out = aacc[...]
        for i in range(count):
            weights = jnp.exp2((sbuf[j + i] - top) * scale)
            total = total + tiles(weights, jnp.add)
            vv = vbuf[pl.ds(2 * (j + i), 2)].reshape(KC, HD)
            out = out + jnp.dot(weights.astype(bf16), vv, preferred_element_type=f32)
        asum[...] = total
        aacc[...] = out

    def attend(t, _):
        m = (c + GROUPS - t) % GROUPS
        for i in range(2):
            src = 2 * m + i

            @pl.when(src != s)
            def _():
                pltpu.make_async_copy(qbuf.at[src], qbuf.at[src], qrecv.at[src]).wait()

        pmax[...] = jnp.full((QG, HD), -BIG, f32)
        asum[...] = jnp.zeros((QG, HD), f32)
        aacc[...] = jnp.zeros((QG, HD), f32)

        def score(j, _):
            first_pass(m, 2 * j, 2)
            return 0

        lax.fori_loop(0, m // 2, score, 0)

        @pl.when(m % 2 == 1)
        def _():
            first_pass(m, m - 1, 1)

        scores = scores_of(m, m)
        row = lax.broadcasted_iota(jnp.int32, (QG, KC), 0)
        row = row + jnp.where(row >= HALF, HALF, 0) + k * HALF
        scores = jnp.where(lax.broadcasted_iota(jnp.int32, (QG, KC), 1) <= row, scores, -BIG)
        sbuf[m] = scores
        highest = jnp.maximum(pmax[...], tiles(scores, jnp.maximum))
        mrow[...] = jnp.broadcast_to(jnp.max(highest, axis=-1, keepdims=True), (QG, HD))

        def step(j, _):
            second_pass(m, 2 * j, 2)
            return 0

        lax.fori_loop(0, (m + 1) // 2, step, 0)

        @pl.when(m % 2 == 0)
        def _():
            second_pass(m, m, 1)

        total = jnp.sum(asum[...], axis=-1, keepdims=True)
        obuf[pl.ds(2 * m, 2)] = (aacc[...] / total).astype(bf16).reshape(2, 8, TOK, HD)

        for i in range(16):
            sp = 2 * m + i // 8
            ei = (e + i) % 8
            copy = remote(obuf.at[sp, ei], tok.at[c, e], osend, orecv.at[c], sp, k * 8 + ei)
            if i % 8:
                copy.start()
                continue
            mine = (sp == s) & (k == e // 8)
            pl.when(jnp.logical_not(mine))(copy.start)

            @pl.when(mine)
            def _():
                pltpu.make_async_copy(obuf.at[sp, ei], tok.at[c, e], orecv.at[c]).start()
                pltpu.make_async_copy(obuf.at[sp, ei], spare, osend).start()

        return 0

    lax.fori_loop(0, GROUPS, attend, 0)

    gain = gain_ref[...]

    def norm(b, _):
        pltpu.make_async_copy(tok.at[b], tok.at[b], orecv.at[b]).wait()
        v = tok[b].astype(f32)
        square = jnp.sum(jnp.sum(v * v, axis=0), axis=-1, keepdims=True)
        spread = jnp.sqrt(square * (1.0 / 2048.0) + 1e-6)
        n = (v / spread[None] * gain[:, None, :]).astype(bf16)
        for h in range(16):
            normed_ref[b, :, h * HD:(h + 1) * HD] = n[h]
            xbuf[b * 4 + h // 4, :, (h % 4) * HD:(h % 4 + 1) * HD] = n[h]
        return 0

    lax.fori_loop(0, SEQS, norm, 0)

    def sending(i):
        return remote(outbuf.at[i], arrived.at[e], dsend.at[i], drecv.at[e], s, partner_to(e, i))

    slot_line = lax.broadcasted_iota(jnp.int32, (ROWS, SUB), 0)

    def gathered(d):
        slot = (slot_line + d * ROWS).astype(f32)
        chosen = ((slot == slot0) | (slot == slot1)).astype(f32).astype(bf16)
        rows = jnp.dot(chosen, xbuf[...].reshape(SUB, SUB), preferred_element_type=f32)
        return rows.astype(bf16).reshape(EPD, CAP, SUB)

    def dispatch(i, _):
        outbuf[i] = gathered(partner_to(e, i))
        sending(i).start()
        return 0

    lax.fori_loop(0, NE - 1, dispatch, 0)
    arrived[e] = gathered(e)

    logits = lax.dot_general(
        xbuf[...].reshape(SUB, SUB), rw_ref[...], (((1,), (1,)), ((), ())), preferred_element_type=f32
    )
    lanes64 = lax.broadcasted_iota(jnp.int32, (SUB, 64), 1).astype(f32)
    picked = [
        jnp.sum(jnp.where(lanes64 == cols[2 + t][:, 0:64], logits, 0.0), axis=1, keepdims=True) for t in range(2)
    ]
    sig0 = 1.0 / (1.0 + jnp.exp(-picked[0]))
    sig1 = 1.0 / (1.0 + jnp.exp(-picked[1]))
    cols[2] = jnp.broadcast_to(sig0 / (sig0 + sig1), (SUB, HD))
    cols[3] = jnp.broadcast_to(sig1 / (sig0 + sig1), (SUB, HD))
    acc[...] = jnp.zeros((SUB, SUB), f32)

    for copy in loads:
        copy.wait()

    def giving(i):
        return remote(res.at[i], returned.at[e], rsend.at[i], rrecv.at[e], s, partner_from(e, i))

    def group(q, _):
        sources = [partner_from(e, q * 4 + j) for j in range(4)]
        for j in range(4):
            src = sources[j]

            @pl.when(src != e)
            def _():
                pltpu.make_async_copy(arrived.at[src], arrived.at[src], drecv.at[src]).wait()

        def one(xp, _):
            a = jnp.concatenate([arrived[src, xp] for src in sources], axis=0)
            u = jnp.dot(a, win[xp], preferred_element_type=f32)
            hid = 0.5 * u * (1.0 + jnp.tanh(0.7978845608028654 * (u + 0.044715 * (u * u * u))))
            y = jnp.dot(hid.astype(bf16), wout[xp], preferred_element_type=f32).astype(bf16)
            for j in range(4):
                res[q * 4 + j, xp] = y[j * CAP:(j + 1) * CAP]
            return 0

        lax.fori_loop(0, EPD, one, 0)
        for j in range(4):
            i = q * 4 + j

            @pl.when(i != NE - 1)
            def _():
                giving(i).start()

        return 0

    lax.fori_loop(0, 4, group, 0)
    returned[e] = res[NE - 1]

    lane = lax.broadcasted_iota(jnp.int32, (SUB, HD), 1)

    def combine(p, _):
        parts = []
        tables = []
        for j in range(2):
            d = partner_to(e, 2 * p + j)

            @pl.when(d != e)
            def _():
                pltpu.make_async_copy(returned.at[d], returned.at[d], rrecv.at[d]).wait()

            slot = (lane + d * ROWS).astype(f32)
            tables.append(
                jnp.where(slot == cols[0], cols[2], 0.0) + jnp.where(slot == cols[1], cols[3], 0.0)
            )
            parts.append(returned[d].reshape(ROWS, SUB))
        table = jnp.concatenate(tables, axis=1)
        rows = jnp.concatenate(parts, axis=0)
        high = table.astype(bf16)
        low = (table - high.astype(f32)).astype(bf16)
        acc[...] += jnp.dot(high, rows, preferred_element_type=f32) + jnp.dot(low, rows, preferred_element_type=f32)
        return 0

    lax.fori_loop(0, NE // 2, combine, 0)
    for b in range(SEQS):
        for g in range(4):
            mix_ref[b, :, g * SUB:(g + 1) * SUB] = acc[(b * 4 + g) * TOK:(b * 4 + g + 1) * TOK].astype(bf16)

    pltpu.make_async_copy(obuf, obuf, osend).wait()

    def drain(j, _):
        for i in range(4):
            send(i, j).wait_send()
        for i in range(2):
            forward(i, j).wait_send()
        return 0

    lax.fori_loop(1, SEQS, drain, 0)
    for copy in near:
        copy.wait_send()

    def drain_rows(i, _):
        sending(i).wait_send()
        giving(i).wait_send()
        return 0

    lax.fori_loop(0, NE - 1, drain_rows, 0)


def body(queries, keys, values, seg_ids, norm_gain, router_w, expert_ids, w_in, w_out):
    ids = expert_ids.transpose(1, 2, 3, 0).reshape(32, 2, TOK)
    vmem = pl.BlockSpec(memory_space=pltpu.VMEM)
    hbm = pl.BlockSpec(memory_space=pl.ANY)
    dma = pltpu.SemaphoreType.DMA
    bf16, f32 = jnp.bfloat16, jnp.float32
    return pl.pallas_call(
        kernel,
        out_shape=(
            jax.ShapeDtypeStruct((SEQS, TOK, 2048), bf16),
            jax.ShapeDtypeStruct((SEQS, TOK, 2048), bf16),
        ),
        in_specs=[hbm] * 3 + [vmem] * 4 + [hbm] * 2,
        out_specs=(vmem, vmem),
        scratch_shapes=[
            pltpu.VMEM((NS, HALF, HD), bf16),
            pltpu.VMEM((NS, BLK, HD), bf16),
            pltpu.VMEM((NS, BLK, HD), bf16),
            pltpu.VMEM((GROUPS, QG, HD), bf16),
            pltpu.VMEM((GROUPS, KC, HD), bf16),
            pltpu.VMEM((GROUPS, QG, KC), f32),
            pltpu.VMEM((QG, HD), f32),
            pltpu.VMEM((QG, HD), f32),
            pltpu.VMEM((QG, HD), f32),
            pltpu.VMEM((QG, HD), f32),
            pltpu.VMEM((NS, 8, TOK, HD), bf16),
            pltpu.VMEM((SEQS, NE, TOK, HD), bf16),
            pltpu.VMEM((32, TOK, SUB), bf16),
            pltpu.VMEM((NE, EPD, CAP, SUB), bf16),
            pltpu.VMEM((NE, EPD, CAP, SUB), bf16),
            pltpu.VMEM((NE, EPD, CAP, SUB), bf16),
            pltpu.VMEM((NE, EPD, CAP, SUB), bf16),
            pltpu.VMEM((EPD, SUB, FFH), bf16),
            pltpu.VMEM((EPD, FFH, SUB), bf16),
            pltpu.VMEM((SUB, SUB), f32),
            pltpu.VMEM((4, SUB, HD), f32),
            pltpu.VMEM((TOK, HD), bf16),
            pltpu.SemaphoreType.REGULAR,
            dma((3,)), dma((SEQS,)), dma((SEQS,)), dma((2 * SEQS,)),
            dma((NS,)), dma((NS,)), dma((NS,)), dma((SEQS,)), dma((SEQS,)),
            dma((2,)), dma(()), dma((SEQS,)), dma((NE,)), dma((NE,)), dma((NE,)), dma((NE,)),
        ],
        compiler_params=pltpu.CompilerParams(
            collective_id=0, has_side_effects=True, vmem_limit_bytes=56 * 1024 * 1024
        ),
        name="block",
    )(
        queries.reshape(SEQS, 2, HALF, HD), keys, values, seg_ids, ids,
        norm_gain.reshape(16, HD), router_w.T, w_in, w_out,
    )


def solution(mesh):
    return jax.shard_map(
        body,
        mesh=mesh,
        in_specs=(
            P(None, "seq", "exp"),
            P(None, "seq", "exp"),
            P(None, "seq", "exp"),
            P(),
            P(),
            P(),
            P(("seq", "exp"), None, None, None),
            P("exp", None, None),
            P("exp", None, None),
        ),
        out_specs=(P(None, ("seq", "exp"), None), P(None, ("seq", "exp"), None)),
        check_vma=False,
    )
```

```python
import functools

import jax
import jax.numpy as jnp
from jax import lax
from jax.experimental import pallas as pl
from jax.experimental.pallas import tpu as pltpu
from jax.sharding import PartitionSpec as P

HD = 128
SUB = 512
CAP = 32
NEG = -1e30
LOG2E = 1.4426950408889634

NS = 16
NE = 16
SEQS = 8
BLK = 256
HALF = 128
EPD = 4
ROWS = EPD * CAP
FFH = 1024
TOK = 16

QG = 256
KC = 512
GROUPS = 8
BIG = 2.0**100
MESH = pl.DeviceIdType.MESH


def other(seq, exp):
    return {"seq": seq, "exp": exp}


def offset_of(i):
    p = i // 2
    mag = 4 - (p + 1) // 2
    return (i + 1) % 2, jnp.where(p % 2 == 0, NZ - mag, mag)


NZ = 8


def partner_to(e, i):
    dy, dz = offset_of(i)
    return (e // NZ + dy) % 2 * NZ + (e % NZ + dz) % NZ


def partner_from(e, i):
    dy, dz = offset_of(i)
    return (e // NZ + dy) % 2 * NZ + (e % NZ + NZ - dz) % NZ


def region(i):
    if isinstance(i, int) and i < 2:
        return 2 * i, 2
    if isinstance(i, int) and i == NE:
        return 60, 2
    return EPD * (i - 1), EPD


def experts_of(e, chunk):
    def of(i):
        d = partner_to(e, i)
        y, z = d // NZ, d % NZ
        return EPD * d, EPD * (y * NZ + (z + NZ - 1) % NZ), EPD * (y * NZ + (z + 1) % NZ)

    if isinstance(chunk, int) and chunk == 0:
        first, second = of(0)[0], of(1)[0]
        return first + 2, first + 3, second + 2, second + 3
    if isinstance(chunk, int) and chunk == NE - 1:
        (first, before, _), (second, before2, _) = of(NE - 2), of(NE - 1)
        return first + 1, before, second + 1, before2
    i = chunk + 1
    home, before, after = of(i)
    up = (i // 2) % 2 == 1
    return home + 2, home + 3, jnp.where(up, home, home + 1), jnp.where(up, after + 1, before)


def kernel(
    q_ref, k_ref, v_ref, seg_ref, ids_ref, gain_ref, rw_ref, win_hbm, wout_hbm, normed_ref, mix_ref,
    qbuf, kbuf, vbuf, qaug, kaug, sbuf, pmax, mrow, asum, aacc, obuf,
    tok, xbuf, outbuf, arrived, res, returned, win, wout, acc, cols, spare,
    ready, loc, ksend, vsend, qsend, krecv, vrecv, qrecv, kfwd, vfwd,
    wsem, osend, orecv, dsend, drecv, rsend, rrecv, wsend, wrecv, wsend2,
):
    s = lax.axis_index("seq")
    e = lax.axis_index("exp")
    c = s // 2
    k = s % 2
    other_core = 2 * c + 1 - k
    f32, bf16 = jnp.float32, jnp.bfloat16

    loads = (
        pltpu.make_async_copy(win_hbm, win.at[pl.ds(0, EPD)], wsem.at[0]),
        pltpu.make_async_copy(wout_hbm, wout.at[pl.ds(0, EPD)], wsem.at[1]),
    )

    barrier = pltpu.get_barrier_semaphore()

    def greet(i, _):
        pl.semaphore_signal(barrier, inc=1, device_id=other((s + i) % NS, e), device_id_type=MESH)
        pl.semaphore_signal(barrier, inc=1, device_id=other(s, (e + i) % NE), device_id_type=MESH)
        return 0

    lax.fori_loop(1, NS, greet, 0)
    pl.semaphore_wait(barrier, 2 * (NS - 1))

    def remote(src, dst, ss, rs, seq, exp):
        return pltpu.make_async_remote_copy(
            src_ref=src, dst_ref=dst, send_sem=ss, recv_sem=rs, device_id=other(seq, exp), device_id_type=MESH
        )

    def send(which, j):
        b = (c + j) % SEQS
        same = 2 * b + k
        cross = 2 * b + 1 - k
        if which == 0:
            return remote(k_ref.at[b], kbuf.at[s], ksend.at[j], krecv.at[s], same, e)
        if which == 1:
            return remote(q_ref.at[b, k], qbuf.at[s], qsend.at[j], qrecv.at[s], same, e)
        if which == 2:
            return remote(q_ref.at[b, 1 - k], qbuf.at[s], qsend.at[SEQS + j], qrecv.at[s], cross, e)
        return remote(v_ref.at[b], vbuf.at[s], vsend.at[j], vrecv.at[s], same, e)

    def start_with(*which):
        def start(j, _):
            for i in which:
                send(i, j).start()
            return 0

        lax.fori_loop(1, SEQS, start, 0)

    def copy_weights(part, j):
        src, dst = (win_hbm, win) if part == 0 else (wout_hbm, wout)
        z = (e % NZ + (1 if j == 0 else NZ - 1)) % NZ
        return remote(src.at[j], dst.at[EPD + j], wsend.at[j], wrecv.at[part, j], s, e // NZ * NZ + z)

    def pass_weights(part, j):
        buf = win if part == 0 else wout
        return remote(buf.at[EPD + j], buf.at[EPD + j], wsend2.at[j], wrecv.at[part, j], other_core, e)

    for part in range(2):

        @pl.when(k == part)
        def _():
            copy_weights(part, 0).start()
            copy_weights(part, 1).start()

    start_with(0)
    own = (
        pltpu.make_async_copy(k_ref.at[c], kbuf.at[s], loc.at[0]),
        pltpu.make_async_copy(v_ref.at[c], vbuf.at[s], loc.at[1]),
        pltpu.make_async_copy(q_ref.at[c, k], qbuf.at[s], loc.at[2]),
    )
    near = (
        remote(k_ref.at[c], kbuf.at[s], kfwd.at[0], krecv.at[s], other_core, e),
        remote(v_ref.at[c], vbuf.at[s], vfwd.at[0], vrecv.at[s], other_core, e),
        remote(q_ref.at[c, 1 - k], qbuf.at[s], qsend.at[0], qrecv.at[s], other_core, e),
    )
    for copy in own + near:
        copy.start()
    start_with(3)
    start_with(1, 2)
    for copy in loads:
        copy.start()

    def greet_again(i, _):
        pl.semaphore_signal(ready, inc=1, device_id=other(s, (e + i) % NE), device_id_type=MESH)
        return 0

    lax.fori_loop(1, NE, greet_again, 0)

    seg = seg_ref[pl.ds(c, 1), :]
    firsts = [jnp.sum((seg < v).astype(jnp.int32)) for v in (1, 2, 3)]

    def document(pos):
        return sum((pos >= f).astype(jnp.int32) for f in firsts)

    def mark(j, _):
        key_pos = lax.broadcasted_iota(jnp.int32, (KC, HD), 0) + j * KC
        lane = lax.broadcasted_iota(jnp.int32, (KC, HD), 1)
        kaug[j] = (document(key_pos) == lane).astype(f32).astype(bf16)
        row = lax.broadcasted_iota(jnp.int32, (QG, HD), 0)
        query_pos = row + jnp.where(row >= HALF, HALF, 0) + (j * KC + k * HALF)
        lane = lax.broadcasted_iota(jnp.int32, (QG, HD), 1)
        qaug[j] = jnp.where(document(query_pos) == lane, 0.0, -BIG).astype(bf16)
        return 0

    lax.fori_loop(0, GROUPS, mark, 0)

    to_lane = (
        lax.broadcasted_iota(jnp.int32, (TOK, SUB), 0) == lax.broadcasted_iota(jnp.int32, (TOK, SUB), 1) % TOK
    ).astype(f32).astype(bf16)
    own_row = lax.broadcasted_iota(jnp.int32, (32, SUB), 0) == lax.broadcasted_iota(jnp.int32, (32, SUB), 1) // TOK
    ids = []
    for t in range(2):
        table = jnp.dot(ids_ref[:, t, :].astype(f32).astype(bf16), to_lane, preferred_element_type=f32)
        ids.append(jnp.sum(jnp.where(own_row, table, 0.0), axis=0, keepdims=True))
    experts = lax.broadcasted_iota(jnp.int32, (64, SUB), 0).astype(f32)
    before = (
        lax.broadcasted_iota(jnp.int32, (SUB, SUB), 0) < lax.broadcasted_iota(jnp.int32, (SUB, SUB), 1)
    ).astype(f32).astype(bf16)
    hot0 = (experts == ids[0]).astype(f32)
    hot1 = (experts == ids[1]).astype(f32)
    run0 = jnp.dot(hot0.astype(bf16), before, preferred_element_type=f32)
    run1 = jnp.dot(hot1.astype(bf16), before, preferred_element_type=f32)
    run1 = run1 + jnp.sum(hot0, axis=1, keepdims=True)
    slot0 = ids[0] * CAP + jnp.sum(run0 * hot0, axis=0, keepdims=True)
    slot1 = ids[1] * CAP + jnp.sum(run1 * hot1, axis=0, keepdims=True)
    lines = jnp.concatenate([slot0, slot1, *ids, jnp.zeros((124, SUB), f32)], axis=0)
    lines = jnp.transpose(lines)
    for i in range(4):
        cols[i] = jnp.broadcast_to(lines[:, i:i + 1], (SUB, HD))

    def forward(which, j):
        src = 2 * ((c + SEQS - j) % SEQS) + k
        if which == 0:
            return remote(kbuf.at[src], kbuf.at[src], kfwd.at[j], krecv.at[src], other_core, e)
        return remote(vbuf.at[src], vbuf.at[src], vfwd.at[j], vrecv.at[src], other_core, e)

    def relay_of(which):
        def relay(j, _):
            copy = forward(which, j)
            copy.wait_recv()
            copy.start()
            return 0

        lax.fori_loop(1, SEQS, relay, 0)

    def finish_of(buf, sem):
        def finish(j, _):
            src = 2 * ((c + SEQS - j) % SEQS) + 1 - k
            pltpu.make_async_copy(buf.at[src], buf.at[src], sem.at[src]).wait()
            return 0

        lax.fori_loop(0, SEQS, finish, 0)

    relay_of(0)
    relay_of(1)
    finish_of(kbuf, krecv)
    finish_of(vbuf, vrecv)
    for copy in own:
        copy.wait()
    pl.semaphore_wait(ready, NE - 1)

    scale = HD ** (-0.5) * LOG2E

    def scores_of(m, j):
        qq = jnp.concatenate([qbuf[pl.ds(2 * m, 2)].reshape(QG, HD), qaug[m]], axis=1)
        kk = jnp.concatenate([kbuf[pl.ds(2 * j, 2)].reshape(KC, HD), kaug[j]], axis=1)
        return lax.dot_general(qq, kk, (((1,), (1,)), ((), ())), preferred_element_type=f32)

    def tiles(x, op):
        out = x[:, 0:HD]
        for i in range(1, KC // HD):
            out = op(out, x[:, i * HD:(i + 1) * HD])
        return out

    def first_pass(m, j, count):
        highest = pmax[...]
        for i in range(count):
            scores = scores_of(m, j + i)
            sbuf[j + i] = scores
            highest = jnp.maximum(highest, tiles(scores, jnp.maximum))
        pmax[...] = highest

    def second_pass(m, j, count):
        top = jnp.concatenate([mrow[...]] * (KC // HD), axis=1)
        total = asum[...]
        out = aacc[...]
        for i in range(count):
            weights = jnp.exp2((sbuf[j + i] - top) * scale)
            total = total + tiles(weights, jnp.add)
            vv = vbuf[pl.ds(2 * (j + i), 2)].reshape(KC, HD)
            out = out + jnp.dot(weights.astype(bf16), vv, preferred_element_type=f32)
        asum[...] = total
        aacc[...] = out

    def attend(t, _):
        m = (c + GROUPS - t) % GROUPS
        for i in range(2):
            src = 2 * m + i

            @pl.when(src != s)
            def _():
                pltpu.make_async_copy(qbuf.at[src], qbuf.at[src], qrecv.at[src]).wait()

        pmax[...] = jnp.full((QG, HD), -BIG, f32)
        asum[...] = jnp.zeros((QG, HD), f32)
        aacc[...] = jnp.zeros((QG, HD), f32)

        def score(j, _):
            first_pass(m, 2 * j, 2)
            return 0

        lax.fori_loop(0, m // 2, score, 0)

        @pl.when(m % 2 == 1)
        def _():
            first_pass(m, m - 1, 1)

        scores = scores_of(m, m)
        row = lax.broadcasted_iota(jnp.int32, (QG, KC), 0)
        row = row + jnp.where(row >= HALF, HALF, 0) + k * HALF
        scores = jnp.where(lax.broadcasted_iota(jnp.int32, (QG, KC), 1) <= row, scores, -BIG)
        sbuf[m] = scores
        highest = jnp.maximum(pmax[...], tiles(scores, jnp.maximum))
        mrow[...] = jnp.broadcast_to(jnp.max(highest, axis=-1, keepdims=True), (QG, HD))

        def step(j, _):
            second_pass(m, 2 * j, 2)
            return 0

        lax.fori_loop(0, (m + 1) // 2, step, 0)

        @pl.when(m % 2 == 0)
        def _():
            second_pass(m, m, 1)

        total = jnp.sum(asum[...], axis=-1, keepdims=True)
        obuf[pl.ds(2 * m, 2)] = (aacc[...] / total).astype(bf16).reshape(2, 8, TOK, HD)

        for i in range(16):
            sp = 2 * m + i // 8
            ei = (e + i) % 8
            copy = remote(obuf.at[sp, ei], tok.at[c, e], osend, orecv.at[c], sp, k * 8 + ei)
            if i % 8:
                copy.start()
                continue
            mine = (sp == s) & (k == e // 8)
            pl.when(jnp.logical_not(mine))(copy.start)

            @pl.when(mine)
            def _():
                pltpu.make_async_copy(obuf.at[sp, ei], tok.at[c, e], orecv.at[c]).start()
                pltpu.make_async_copy(obuf.at[sp, ei], spare, osend).start()

        return 0

    lax.fori_loop(0, GROUPS, attend, 0)

    for part in range(2):

        @pl.when(k == part)
        def _():
            for j in range(2):
                copy = pass_weights(part, j)
                copy.wait_recv()
                copy.start()

    gain = gain_ref[...]

    def norm(b, _):
        pltpu.make_async_copy(tok.at[b], tok.at[b], orecv.at[b]).wait()
        v = tok[b].astype(f32)
        square = jnp.sum(jnp.sum(v * v, axis=0), axis=-1, keepdims=True)
        spread = jnp.sqrt(square * (1.0 / 2048.0) + 1e-6)
        n = (v / spread[None] * gain[:, None, :]).astype(bf16)
        for h in range(16):
            normed_ref[b, :, h * HD:(h + 1) * HD] = n[h]
            xbuf[b * 4 + h // 4, :, (h % 4) * HD:(h % 4 + 1) * HD] = n[h]
        return 0

    lax.fori_loop(0, SEQS, norm, 0)

    def rows_at(buf, i):
        first, count = region(i)
        return buf.at[pl.ds(first, count)]

    def sending(i):
        return remote(
            rows_at(outbuf, i), rows_at(arrived, i), dsend.at[i], drecv.at[i], s, partner_to(e, 14 if isinstance(i, int) and i == NE else i)
        )

    slot_line = lax.broadcasted_iota(jnp.int32, (CAP, SUB), 0)

    def gathered(chunk):
        slot = jnp.concatenate([slot_line + x * CAP for x in experts_of(e, chunk)], axis=0).astype(f32)
        chosen = ((slot == slot0) | (slot == slot1)).astype(f32).astype(bf16)
        rows = jnp.dot(chosen, xbuf[...].reshape(SUB, SUB), preferred_element_type=f32)
        return rows.astype(bf16).reshape(EPD, CAP, SUB)

    outbuf[0:EPD] = gathered(0)
    sending(0).start()
    sending(1).start()

    def dispatch(i, _):
        outbuf[pl.ds(EPD * (i - 1), EPD)] = gathered(i - 1)
        sending(i).start()
        return 0

    lax.fori_loop(2, NE - 1, dispatch, 0)
    rest = gathered(NE - 1)
    outbuf[60:62] = rest[0:2]
    sending(NE).start()
    arrived[62:64] = rest[2:4]
    arrived[56:60] = gathered(NE - 2)

    logits = lax.dot_general(
        xbuf[...].reshape(SUB, SUB), rw_ref[...], (((1,), (1,)), ((), ())), preferred_element_type=f32
    )
    lanes64 = lax.broadcasted_iota(jnp.int32, (SUB, 64), 1).astype(f32)
    picked = [
        jnp.sum(jnp.where(lanes64 == cols[2 + t][:, 0:64], logits, 0.0), axis=1, keepdims=True) for t in range(2)
    ]
    sig0 = 1.0 / (1.0 + jnp.exp(-picked[0]))
    sig1 = 1.0 / (1.0 + jnp.exp(-picked[1]))
    cols[2] = jnp.broadcast_to(sig0 / (sig0 + sig1), (SUB, HD))
    cols[3] = jnp.broadcast_to(sig1 / (sig0 + sig1), (SUB, HD))
    acc[...] = jnp.zeros((SUB, SUB), f32)

    for copy in loads:
        copy.wait()
    for part in range(2):

        @pl.when(k != part)
        def _():
            for j in range(2):
                buf = (win if part == 0 else wout).at[EPD + j]
                pltpu.make_async_copy(buf, buf, wrecv.at[part, j]).wait()

    def giving(i):
        return remote(
            rows_at(res, i), rows_at(returned, i), rsend.at[i], rrecv.at[i], s, partner_from(e, 14 if isinstance(i, int) and i == NE else i)
        )

    def run_experts(blocks, first, step):
        def one(xp, _):
            w = first + step * xp
            a = jnp.concatenate([arrived[at + xp] for at in blocks], axis=0)
            u = jnp.dot(a, win[w], preferred_element_type=f32)
            hid = 0.5 * u * (1.0 + jnp.tanh(0.7978845608028654 * (u + 0.044715 * (u * u * u))))
            y = jnp.dot(hid.astype(bf16), wout[w], preferred_element_type=f32).astype(bf16)
            for j in range(4):
                res[blocks[j] + xp] = y[j * CAP:(j + 1) * CAP]
            return 0

        lax.fori_loop(0, 2, one, 0)

    plan = (
        ((0, 1, 2, 3, 6, 7), (0, 2, 4, 8), (6, 10, 22, 26), (0, 1, 2, 3)),
        ((4, 5, 8, 9), (12, 16, 20, 24), (14, 18, 30, 34), (4, 5, 6, 7)),
        ((10, 11, 14), (28, 32, 36, 40), (38, 42, 54, 58), (8, 9, 10, 11)),
        ((12, 13, 16), (44, 48, 52, 56), (46, 50, 60, 62), (12, 13, 14, 16)),
    )
    for q, (needed, always, shared, done) in enumerate(plan):
        for i in needed:
            part = rows_at(arrived, i)
            pltpu.make_async_copy(part, part, drecv.at[i]).wait()
        run_experts(always, 2, 1)
        if q % 2 == 0:
            run_experts(shared, 0, 5)
        else:
            run_experts(shared, 1, 3)
        for i in done:
            giving(i).start()
    returned[56:60] = res[56:60]
    returned[62:64] = res[62:64]

    lane = lax.broadcasted_iota(jnp.int32, (SUB, HD), 1)

    def table_of(chunk):
        x = experts_of(e, chunk)
        part = lane // CAP
        slot = jnp.where(part < 2, jnp.where(part == 0, x[0], x[1]), jnp.where(part == 2, x[2], x[3]))
        slot = (slot * CAP + lane % CAP).astype(f32)
        return jnp.where(slot == cols[0], cols[2], 0.0) + jnp.where(slot == cols[1], cols[3], 0.0)

    def add_rows(tables, parts):
        table = jnp.concatenate(tables, axis=1)
        rows = jnp.concatenate(parts, axis=0)
        high = table.astype(bf16)
        low = (table - high.astype(f32)).astype(bf16)
        acc[...] += jnp.dot(high, rows, preferred_element_type=f32) + jnp.dot(low, rows, preferred_element_type=f32)

    def chunk_rows(chunk):
        return returned[pl.ds(EPD * chunk, EPD)].reshape(ROWS, SUB)

    def wait_rows(i):
        part = rows_at(returned, i)
        pltpu.make_async_copy(part, part, rrecv.at[i]).wait()

    for i in (0, 1, 2):
        wait_rows(i)
    add_rows([table_of(0), table_of(1)], [chunk_rows(0), chunk_rows(1)])

    def combine(p, _):
        wait_rows(2 * p + 1)
        wait_rows(2 * p + 2)
        add_rows([table_of(2 * p), table_of(2 * p + 1)], [chunk_rows(2 * p), chunk_rows(2 * p + 1)])
        return 0

    lax.fori_loop(1, NE // 2 - 1, combine, 0)
    wait_rows(NE)
    add_rows([table_of(NE - 2), table_of(NE - 1)], [chunk_rows(NE - 2), chunk_rows(NE - 1)])
    for b in range(SEQS):
        for g in range(4):
            mix_ref[b, :, g * SUB:(g + 1) * SUB] = acc[(b * 4 + g) * TOK:(b * 4 + g + 1) * TOK].astype(bf16)

    pltpu.make_async_copy(obuf, obuf, osend).wait()

    def drain(j, _):
        for i in range(4):
            send(i, j).wait_send()
        for i in range(2):
            forward(i, j).wait_send()
        return 0

    lax.fori_loop(1, SEQS, drain, 0)
    for copy in near:
        copy.wait_send()

    def drain_rows(i, _):
        sending(i).wait_send()
        giving(i).wait_send()
        return 0

    for i in (0, 1, NE):
        drain_rows(i, 0)
    lax.fori_loop(2, NE - 1, drain_rows, 0)
    for part in range(2):

        @pl.when(k == part)
        def _():
            for j in range(2):
                copy_weights(part, j).wait_send()
                pass_weights(part, j).wait_send()


def body(queries, keys, values, seg_ids, norm_gain, router_w, expert_ids, w_in, w_out):
    ids = expert_ids.transpose(1, 2, 3, 0).reshape(32, 2, TOK)
    vmem = pl.BlockSpec(memory_space=pltpu.VMEM)
    hbm = pl.BlockSpec(memory_space=pl.ANY)
    dma = pltpu.SemaphoreType.DMA
    bf16, f32 = jnp.bfloat16, jnp.float32
    return pl.pallas_call(
        kernel,
        out_shape=(
            jax.ShapeDtypeStruct((SEQS, TOK, 2048), bf16),
            jax.ShapeDtypeStruct((SEQS, TOK, 2048), bf16),
        ),
        in_specs=[hbm] * 3 + [vmem] * 4 + [hbm] * 2,
        out_specs=(vmem, vmem),
        scratch_shapes=[
            pltpu.VMEM((NS, HALF, HD), bf16),
            pltpu.VMEM((NS, BLK, HD), bf16),
            pltpu.VMEM((NS, BLK, HD), bf16),
            pltpu.VMEM((GROUPS, QG, HD), bf16),
            pltpu.VMEM((GROUPS, KC, HD), bf16),
            pltpu.VMEM((GROUPS, QG, KC), f32),
            pltpu.VMEM((QG, HD), f32),
            pltpu.VMEM((QG, HD), f32),
            pltpu.VMEM((QG, HD), f32),
            pltpu.VMEM((QG, HD), f32),
            pltpu.VMEM((NS, 8, TOK, HD), bf16),
            pltpu.VMEM((SEQS, NE, TOK, HD), bf16),
            pltpu.VMEM((32, TOK, SUB), bf16),
            pltpu.VMEM((NE * EPD, CAP, SUB), bf16),
            pltpu.VMEM((NE * EPD, CAP, SUB), bf16),
            pltpu.VMEM((NE * EPD, CAP, SUB), bf16),
            pltpu.VMEM((NE * EPD, CAP, SUB), bf16),
            pltpu.VMEM((EPD + 2, SUB, FFH), bf16),
            pltpu.VMEM((EPD + 2, FFH, SUB), bf16),
            pltpu.VMEM((SUB, SUB), f32),
            pltpu.VMEM((4, SUB, HD), f32),
            pltpu.VMEM((TOK, HD), bf16),
            pltpu.SemaphoreType.REGULAR,
            dma((3,)), dma((SEQS,)), dma((SEQS,)), dma((2 * SEQS,)),
            dma((NS,)), dma((NS,)), dma((NS,)), dma((SEQS,)), dma((SEQS,)),
            dma((2,)), dma(()), dma((SEQS,)), dma((NE + 1,)), dma((NE + 1,)), dma((NE + 1,)), dma((NE + 1,)),
            dma((2,)), dma((2, 2)), dma((2,)),
        ],
        compiler_params=pltpu.CompilerParams(
            collective_id=0, has_side_effects=True, vmem_limit_bytes=56 * 1024 * 1024
        ),
        name="block",
    )(
        queries.reshape(SEQS, 2, HALF, HD), keys, values, seg_ids, ids,
        norm_gain.reshape(16, HD), router_w.T, w_in, w_out,
    )


def solution(mesh):
    return jax.shard_map(
        body,
        mesh=mesh,
        in_specs=(
            P(None, "seq", "exp"),
            P(None, "seq", "exp"),
            P(None, "seq", "exp"),
            P(),
            P(),
            P(),
            P(("seq", "exp"), None, None, None),
            P("exp", None, None),
            P("exp", None, None),
        ),
        out_specs=(P(None, ("seq", "exp"), None), P(None, ("seq", "exp"), None)),
        check_vma=False,
    )
```

```python
import functools

import jax
import jax.numpy as jnp
from jax import lax
from jax.experimental import pallas as pl
from jax.experimental.pallas import tpu as pltpu
from jax.sharding import PartitionSpec as P

HD = 128
SUB = 512
CAP = 32
NEG = -1e30
LOG2E = 1.4426950408889634

NS = 16
NE = 16
SEQS = 8
BLK = 256
HALF = 128
EPD = 4
ROWS = EPD * CAP
FFH = 1024
TOK = 16

QG = 256
KC = 512
GROUPS = 8
BIG = 2.0**100
MESH = pl.DeviceIdType.MESH


def other(seq, exp):
    return {"seq": seq, "exp": exp}


def offset_of(i):
    p = i // 2
    mag = 3 - p // 2
    return (i + 1) % 2, jnp.where(p % 2 == 0, mag, NZ - mag)


NEAR = 12
NZ = 8


def partner_to(e, i):
    dy, dz = offset_of(i)
    return (e // NZ + dy) % 2 * NZ + (e % NZ + dz) % NZ


def partner_from(e, i):
    dy, dz = offset_of(i)
    return (e // NZ + dy) % 2 * NZ + (e % NZ + NZ - dz) % NZ


def region(i):
    return EPD * i, (2 * EPD if isinstance(i, int) and i == NEAR else EPD)


def experts_of(e, chunk):
    i = chunk if not isinstance(chunk, int) or chunk < NEAR else NEAR + (chunk - NEAR) // 2
    d = partner_to(e, i)
    y, z = d // NZ, d % NZ
    home = EPD * d
    before = EPD * (y * NZ + (z + NZ - 1) % NZ)
    after = EPD * (y * NZ + (z + 1) % NZ)
    up = (i // 2) % 2 == 0 if not isinstance(chunk, int) or chunk < NEAR else chunk % 2 == 0
    ahead = (home, home + 2, after + 1, after + 3)
    behind = (home + 1, home + 3, before, before + 2)
    return tuple(jnp.where(up, f, g) for f, g in zip(ahead, behind))


def kernel(
    q_ref, k_ref, v_ref, seg_ref, ids_ref, gain_ref, rw_ref, win_hbm, wout_hbm, normed_ref, mix_ref,
    qbuf, kbuf, vbuf, qaug, kaug, sbuf, pmax, mrow, asum, aacc, obuf,
    tok, xbuf, outbuf, arrived, res, returned, win, wout, acc, cols, spare,
    ready, loc, ksend, vsend, qsend, krecv, vrecv, qrecv, kfwd, vfwd,
    wsem, osend, orecv, dsend, drecv, rsend, rrecv, wsend, wrecv, wsend2, zsend, precv, bsend, fsend, rsend2, rrecv2,
):
    s = lax.axis_index("seq")
    e = lax.axis_index("exp")
    c = s // 2
    k = s % 2
    other_core = 2 * c + 1 - k
    f32, bf16 = jnp.float32, jnp.bfloat16

    loads = (
        pltpu.make_async_copy(win_hbm, win.at[pl.ds(0, EPD)], wsem.at[0]),
        pltpu.make_async_copy(wout_hbm, wout.at[pl.ds(0, EPD)], wsem.at[1]),
    )

    barrier = pltpu.get_barrier_semaphore()

    def greet(i, _):
        pl.semaphore_signal(barrier, inc=1, device_id=other((s + i) % NS, e), device_id_type=MESH)
        pl.semaphore_signal(barrier, inc=1, device_id=other(s, (e + i) % NE), device_id_type=MESH)
        return 0

    lax.fori_loop(1, NS, greet, 0)
    pl.semaphore_wait(barrier, 2 * (NS - 1))

    def remote(src, dst, ss, rs, seq, exp):
        return pltpu.make_async_remote_copy(
            src_ref=src, dst_ref=dst, send_sem=ss, recv_sem=rs, device_id=other(seq, exp), device_id_type=MESH
        )

    def send(which, j):
        b = (c + j) % SEQS
        same = 2 * b + k
        cross = 2 * b + 1 - k
        if which == 0:
            return remote(k_ref.at[b], kbuf.at[s], ksend.at[j], krecv.at[s], same, e)
        if which == 1:
            return remote(q_ref.at[b, k], qbuf.at[s], qsend.at[j], qrecv.at[s], same, e)
        if which == 2:
            return remote(q_ref.at[b, 1 - k], qbuf.at[s], qsend.at[SEQS + j], qrecv.at[s], cross, e)
        return remote(v_ref.at[b], vbuf.at[s], vsend.at[j], vrecv.at[s], same, e)

    def start_with(*which):
        def start(j, _):
            for i in which:
                send(i, j).start()
            return 0

        lax.fori_loop(1, SEQS, start, 0)

    def copy_weights(part, j):
        src, dst = (win_hbm, win) if part == 0 else (wout_hbm, wout)
        z = (e % NZ + (1 if j == 0 else NZ - 1)) % NZ
        return remote(src.at[j], dst.at[EPD + j], wsend.at[j], wrecv.at[part, j], s, e // NZ * NZ + z)

    def pass_weights(part, j):
        buf = win if part == 0 else wout
        return remote(buf.at[EPD + j], buf.at[EPD + j], wsend2.at[j], wrecv.at[part, j], other_core, e)

    def piece_of(part, x, p):
        return (win.at[x, pl.ds(p * 64, 64)], wout.at[x, pl.ds(p * 128, 128)])[part]

    def copy_piece(part, j):
        src = (win_hbm.at[2 + j, pl.ds(c * 64, 64)], wout_hbm.at[2 + j, pl.ds(c * 128, 128)])[part]
        z = (e % NZ + (1 if j == 0 else NZ - 1)) % NZ
        return remote(src, piece_of(part, 6 + j, c), zsend.at[j], precv.at[part, j, c], s, e // NZ * NZ + z)

    def share_piece(part, j, i):
        piece = piece_of(part, 6 + j, c)
        to = other_core if isinstance(i, int) else 2 * ((c + i) % SEQS) + k
        return remote(piece, piece, bsend.at[j, i], precv.at[part, j, c], to, e)

    def pass_piece(part, j, i):
        p = (c + SEQS - i) % SEQS
        piece = piece_of(part, 6 + j, p)
        return remote(piece, piece, fsend.at[j, i], precv.at[part, j, p], other_core, e)

    def on_part(act):
        for part in range(2):
            pl.when(k == part)(functools.partial(act, part))

    def over_pieces(make, act):
        def one(i, _):
            for j in range(2):
                act(make(j, i))
            return 0

        lax.fori_loop(1, SEQS, one, 0)

    def first_weights(part):
        for j in range(2):
            copy_piece(part, j).start()
        for j in range(2):
            copy_weights(part, j).start()

    def share_weights(part):
        for j in range(2):
            copy_piece(part, j).wait_recv()
            share_piece(part, j, 0).start()
        over_pieces(functools.partial(share_piece, part), lambda copy: copy.start())

    def pass_pieces(part):
        def go(copy):
            copy.wait_recv()
            copy.start()

        over_pieces(functools.partial(pass_piece, part), go)

    def take_pieces(part):
        def one(p, _):
            for j in range(2):
                piece = piece_of(1 - part, 6 + j, p)
                pltpu.make_async_copy(piece, piece, precv.at[1 - part, j, p]).wait()
            return 0

        lax.fori_loop(0, SEQS, one, 0)

    def drain_pieces(part):
        for j in range(2):
            copy_piece(part, j).wait_send()
            share_piece(part, j, 0).wait_send()
        over_pieces(functools.partial(share_piece, part), lambda copy: copy.wait_send())
        over_pieces(functools.partial(pass_piece, part), lambda copy: copy.wait_send())

    on_part(first_weights)
    start_with(0)
    own = (
        pltpu.make_async_copy(k_ref.at[c], kbuf.at[s], loc.at[0]),
        pltpu.make_async_copy(v_ref.at[c], vbuf.at[s], loc.at[1]),
        pltpu.make_async_copy(q_ref.at[c, k], qbuf.at[s], loc.at[2]),
    )
    near = (
        remote(k_ref.at[c], kbuf.at[s], kfwd.at[0], krecv.at[s], other_core, e),
        remote(v_ref.at[c], vbuf.at[s], vfwd.at[0], vrecv.at[s], other_core, e),
        remote(q_ref.at[c, 1 - k], qbuf.at[s], qsend.at[0], qrecv.at[s], other_core, e),
    )
    for copy in own + near:
        copy.start()
    start_with(3)
    start_with(1, 2)
    for copy in loads:
        copy.start()

    def greet_again(i, _):
        pl.semaphore_signal(ready, inc=1, device_id=other(s, (e + i) % NE), device_id_type=MESH)
        return 0

    lax.fori_loop(1, NE, greet_again, 0)

    seg = seg_ref[pl.ds(c, 1), :]
    firsts = [jnp.sum((seg < v).astype(jnp.int32)) for v in (1, 2, 3)]

    def document(pos):
        return sum((pos >= f).astype(jnp.int32) for f in firsts)

    def mark(j, _):
        key_pos = lax.broadcasted_iota(jnp.int32, (KC, HD), 0) + j * KC
        lane = lax.broadcasted_iota(jnp.int32, (KC, HD), 1)
        kaug[j] = (document(key_pos) == lane).astype(f32).astype(bf16)
        row = lax.broadcasted_iota(jnp.int32, (QG, HD), 0)
        query_pos = row + jnp.where(row >= HALF, HALF, 0) + (j * KC + k * HALF)
        lane = lax.broadcasted_iota(jnp.int32, (QG, HD), 1)
        qaug[j] = jnp.where(document(query_pos) == lane, 0.0, -BIG).astype(bf16)
        return 0

    lax.fori_loop(0, GROUPS, mark, 0)

    to_lane = (
        lax.broadcasted_iota(jnp.int32, (TOK, SUB), 0) == lax.broadcasted_iota(jnp.int32, (TOK, SUB), 1) % TOK
    ).astype(f32).astype(bf16)
    own_row = lax.broadcasted_iota(jnp.int32, (32, SUB), 0) == lax.broadcasted_iota(jnp.int32, (32, SUB), 1) // TOK
    ids = []
    for t in range(2):
        table = jnp.dot(ids_ref[:, t, :].astype(f32).astype(bf16), to_lane, preferred_element_type=f32)
        ids.append(jnp.sum(jnp.where(own_row, table, 0.0), axis=0, keepdims=True))
    experts = lax.broadcasted_iota(jnp.int32, (64, SUB), 0).astype(f32)
    before = (
        lax.broadcasted_iota(jnp.int32, (SUB, SUB), 0) < lax.broadcasted_iota(jnp.int32, (SUB, SUB), 1)
    ).astype(f32).astype(bf16)
    hot0 = (experts == ids[0]).astype(f32)
    hot1 = (experts == ids[1]).astype(f32)
    run0 = jnp.dot(hot0.astype(bf16), before, preferred_element_type=f32)
    run1 = jnp.dot(hot1.astype(bf16), before, preferred_element_type=f32)
    run1 = run1 + jnp.sum(hot0, axis=1, keepdims=True)
    slot0 = ids[0] * CAP + jnp.sum(run0 * hot0, axis=0, keepdims=True)
    slot1 = ids[1] * CAP + jnp.sum(run1 * hot1, axis=0, keepdims=True)
    lines = jnp.concatenate([slot0, slot1, *ids, jnp.zeros((124, SUB), f32)], axis=0)
    lines = jnp.transpose(lines)
    for i in range(4):
        cols[i] = jnp.broadcast_to(lines[:, i:i + 1], (SUB, HD))

    def forward(which, j):
        src = 2 * ((c + SEQS - j) % SEQS) + k
        if which == 0:
            return remote(kbuf.at[src], kbuf.at[src], kfwd.at[j], krecv.at[src], other_core, e)
        return remote(vbuf.at[src], vbuf.at[src], vfwd.at[j], vrecv.at[src], other_core, e)

    def relay_of(which):
        def relay(j, _):
            copy = forward(which, j)
            copy.wait_recv()
            copy.start()
            return 0

        lax.fori_loop(1, SEQS, relay, 0)

    def finish_of(buf, sem):
        def finish(j, _):
            src = 2 * ((c + SEQS - j) % SEQS) + 1 - k
            pltpu.make_async_copy(buf.at[src], buf.at[src], sem.at[src]).wait()
            return 0

        lax.fori_loop(0, SEQS, finish, 0)

    relay_of(0)
    relay_of(1)
    finish_of(kbuf, krecv)
    finish_of(vbuf, vrecv)
    for copy in own:
        copy.wait()
    pl.semaphore_wait(ready, NE - 1)

    scale = HD ** (-0.5) * LOG2E

    def scores_of(m, j):
        qq = jnp.concatenate([qbuf[pl.ds(2 * m, 2)].reshape(QG, HD), qaug[m]], axis=1)
        kk = jnp.concatenate([kbuf[pl.ds(2 * j, 2)].reshape(KC, HD), kaug[j]], axis=1)
        return lax.dot_general(qq, kk, (((1,), (1,)), ((), ())), preferred_element_type=f32)

    def tiles(x, op):
        out = x[:, 0:HD]
        for i in range(1, KC // HD):
            out = op(out, x[:, i * HD:(i + 1) * HD])
        return out

    def first_pass(m, j, count):
        highest = pmax[...]
        for i in range(count):
            scores = scores_of(m, j + i)
            sbuf[j + i] = scores
            highest = jnp.maximum(highest, tiles(scores, jnp.maximum))
        pmax[...] = highest

    def second_pass(m, j, count):
        top = jnp.concatenate([mrow[...]] * (KC // HD), axis=1)
        total = asum[...]
        out = aacc[...]
        for i in range(count):
            weights = jnp.exp2((sbuf[j + i] - top) * scale)
            total = total + tiles(weights, jnp.add)
            vv = vbuf[pl.ds(2 * (j + i), 2)].reshape(KC, HD)
            out = out + jnp.dot(weights.astype(bf16), vv, preferred_element_type=f32)
        asum[...] = total
        aacc[...] = out

    def attend(t, _):
        m = (c + GROUPS - t) % GROUPS
        for i in range(2):
            src = 2 * m + i

            @pl.when(src != s)
            def _():
                pltpu.make_async_copy(qbuf.at[src], qbuf.at[src], qrecv.at[src]).wait()

        pmax[...] = jnp.full((QG, HD), -BIG, f32)
        asum[...] = jnp.zeros((QG, HD), f32)
        aacc[...] = jnp.zeros((QG, HD), f32)

        def score(j, _):
            first_pass(m, 2 * j, 2)
            return 0

        lax.fori_loop(0, m // 2, score, 0)

        @pl.when(m % 2 == 1)
        def _():
            first_pass(m, m - 1, 1)

        scores = scores_of(m, m)
        row = lax.broadcasted_iota(jnp.int32, (QG, KC), 0)
        row = row + jnp.where(row >= HALF, HALF, 0) + k * HALF
        scores = jnp.where(lax.broadcasted_iota(jnp.int32, (QG, KC), 1) <= row, scores, -BIG)
        sbuf[m] = scores
        highest = jnp.maximum(pmax[...], tiles(scores, jnp.maximum))
        mrow[...] = jnp.broadcast_to(jnp.max(highest, axis=-1, keepdims=True), (QG, HD))

        def step(j, _):
            second_pass(m, 2 * j, 2)
            return 0

        lax.fori_loop(0, (m + 1) // 2, step, 0)

        @pl.when(m % 2 == 0)
        def _():
            second_pass(m, m, 1)

        total = jnp.sum(asum[...], axis=-1, keepdims=True)
        obuf[pl.ds(2 * m, 2)] = (aacc[...] / total).astype(bf16).reshape(2, 8, TOK, HD)

        for i in range(16):
            sp = 2 * m + i // 8
            ei = (e + i) % 8
            copy = remote(obuf.at[sp, ei], tok.at[c, e], osend, orecv.at[c], sp, k * 8 + ei)
            if i % 8:
                copy.start()
                continue
            mine = (sp == s) & (k == e // 8)
            pl.when(jnp.logical_not(mine))(copy.start)

            @pl.when(mine)
            def _():
                pltpu.make_async_copy(obuf.at[sp, ei], tok.at[c, e], orecv.at[c]).start()
                pltpu.make_async_copy(obuf.at[sp, ei], spare, osend).start()

        return 0

    lax.fori_loop(0, GROUPS, attend, 0)

    on_part(share_weights)

    for part in range(2):

        @pl.when(k == part)
        def _():
            for j in range(2):
                copy = pass_weights(part, j)
                copy.wait_recv()
                copy.start()

    gain = gain_ref[...]

    def norm(b, _):
        pltpu.make_async_copy(tok.at[b], tok.at[b], orecv.at[b]).wait()
        v = tok[b].astype(f32)
        square = jnp.sum(jnp.sum(v * v, axis=0), axis=-1, keepdims=True)
        spread = jnp.sqrt(square * (1.0 / 2048.0) + 1e-6)
        n = (v / spread[None] * gain[:, None, :]).astype(bf16)
        for h in range(16):
            normed_ref[b, :, h * HD:(h + 1) * HD] = n[h]
            xbuf[b * 4 + h // 4, :, (h % 4) * HD:(h % 4 + 1) * HD] = n[h]
        return 0

    lax.fori_loop(0, SEQS, norm, 0)

    def rows_at(buf, i):
        first, count = region(i)
        return buf.at[pl.ds(first, count)]

    def sending(i):
        return remote(rows_at(outbuf, i), rows_at(arrived, i), dsend.at[i], drecv.at[i], s, partner_to(e, i))

    slot_line = lax.broadcasted_iota(jnp.int32, (CAP, SUB), 0)

    def gathered(chunk):
        slot = jnp.concatenate([slot_line + x * CAP for x in experts_of(e, chunk)], axis=0).astype(f32)
        chosen = ((slot == slot0) | (slot == slot1)).astype(f32).astype(bf16)
        rows = jnp.dot(chosen, xbuf[...].reshape(SUB, SUB), preferred_element_type=f32)
        return rows.astype(bf16).reshape(EPD, CAP, SUB)

    def dispatch(i, _):
        outbuf[pl.ds(EPD * i, EPD)] = gathered(i)
        sending(i).start()
        return 0

    lax.fori_loop(0, NEAR, dispatch, 0)
    outbuf[48:52] = gathered(12)
    outbuf[52:56] = gathered(13)
    sending(NEAR).start()
    arrived[56:60] = gathered(14)
    arrived[60:64] = gathered(15)

    logits = lax.dot_general(
        xbuf[...].reshape(SUB, SUB), rw_ref[...], (((1,), (1,)), ((), ())), preferred_element_type=f32
    )
    lanes64 = lax.broadcasted_iota(jnp.int32, (SUB, 64), 1).astype(f32)
    picked = [
        jnp.sum(jnp.where(lanes64 == cols[2 + t][:, 0:64], logits, 0.0), axis=1, keepdims=True) for t in range(2)
    ]
    sig0 = 1.0 / (1.0 + jnp.exp(-picked[0]))
    sig1 = 1.0 / (1.0 + jnp.exp(-picked[1]))
    cols[2] = jnp.broadcast_to(sig0 / (sig0 + sig1), (SUB, HD))
    cols[3] = jnp.broadcast_to(sig1 / (sig0 + sig1), (SUB, HD))
    acc[...] = jnp.zeros((SUB, SUB), f32)

    for copy in loads:
        copy.wait()
    for part in range(2):

        @pl.when(k != part)
        def _():
            for j in range(2):
                buf = (win if part == 0 else wout).at[EPD + j]
                pltpu.make_async_copy(buf, buf, wrecv.at[part, j]).wait()

    def giving(chunk, late):
        i = jnp.minimum(chunk, NEAR)
        first, count = (EPD * chunk + 3, 1) if late else (EPD * chunk, 3)
        return remote(
            res.at[pl.ds(first, count)], returned.at[pl.ds(first, count)],
            (rsend2 if late else rsend).at[chunk], (rrecv2 if late else rrecv).at[chunk], s, partner_from(e, i),
        )

    def run_expert(chunks, xp, w):
        a = jnp.concatenate([arrived[EPD * at + xp] for at in chunks], axis=0)
        u = jnp.dot(a, win[w], preferred_element_type=f32)
        hid = 0.5 * u * (1.0 + jnp.tanh(0.7978845608028654 * (u + 0.044715 * (u * u * u))))
        y = jnp.dot(hid.astype(bf16), wout[w], preferred_element_type=f32).astype(bf16)
        for j in range(4):
            res[EPD * chunks[j] + xp] = y[j * CAP:(j + 1) * CAP]

    plan = (
        ((0, 1, 4, 5), (0, 1, 4, 5), True),
        ((2, 3, 6, 7), (2, 3, 6, 7), False),
        ((8, 9, 12), (8, 9, 12, 14), True),
        ((10, 11), (10, 11, 13, 15), False),
    )
    for needed, chunks, up in plan:
        for i in needed:
            part = rows_at(arrived, i)
            pltpu.make_async_copy(part, part, drecv.at[i]).wait()

        def early(xp, _):
            late = jnp.where(xp >= 2, 1, 0)
            run_expert(chunks, xp, 2 * xp + late if up else 2 * xp + 1 - late)
            return 0

        lax.fori_loop(0, 3, early, 0)
        for chunk in chunks:
            if chunk < 14:
                giving(chunk, False).start()

    on_part(pass_pieces)
    on_part(take_pieces)
    for _, chunks, up in plan:
        run_expert(chunks, 3, 7 if up else 6)
        for chunk in chunks:
            if chunk < 14:
                giving(chunk, True).start()
    returned[56:64] = res[56:64]

    lane = lax.broadcasted_iota(jnp.int32, (SUB, HD), 1)

    def table_of(chunk):
        x = experts_of(e, chunk)
        part = lane // CAP
        slot = jnp.where(part < 2, jnp.where(part == 0, x[0], x[1]), jnp.where(part == 2, x[2], x[3]))
        slot = (slot * CAP + lane % CAP).astype(f32)
        return jnp.where(slot == cols[0], cols[2], 0.0) + jnp.where(slot == cols[1], cols[3], 0.0)

    def add_rows(tables, parts):
        table = jnp.concatenate(tables, axis=1)
        rows = jnp.concatenate(parts, axis=0)
        high = table.astype(bf16)
        low = (table - high.astype(f32)).astype(bf16)
        acc[...] += jnp.dot(high, rows, preferred_element_type=f32) + jnp.dot(low, rows, preferred_element_type=f32)

    def chunk_rows(chunk):
        return returned[pl.ds(EPD * chunk, EPD)].reshape(ROWS, SUB)

    def wait_rows(chunk):
        for first, count, sem in ((EPD * chunk, 3, rrecv), (EPD * chunk + 3, 1, rrecv2)):
            part = returned.at[pl.ds(first, count)]
            pltpu.make_async_copy(part, part, sem.at[chunk]).wait()

    add_rows([table_of(14), table_of(15)], [chunk_rows(14), chunk_rows(15)])

    def combine(a, b):
        wait_rows(a)
        wait_rows(b)
        add_rows([table_of(a), table_of(b)], [chunk_rows(a), chunk_rows(b)])

    for first in (0, 4, 2, 6, 8):
        combine(first, first + 1)
    combine(10, 11)
    combine(12, 13)
    for b in range(SEQS):
        for g in range(4):
            mix_ref[b, :, g * SUB:(g + 1) * SUB] = acc[(b * 4 + g) * TOK:(b * 4 + g + 1) * TOK].astype(bf16)

    pltpu.make_async_copy(obuf, obuf, osend).wait()

    def drain(j, _):
        for i in range(4):
            send(i, j).wait_send()
        for i in range(2):
            forward(i, j).wait_send()
        return 0

    lax.fori_loop(1, SEQS, drain, 0)
    for copy in near:
        copy.wait_send()

    def drain_rows(i, _):
        sending(i).wait_send()
        return 0

    lax.fori_loop(0, NEAR, drain_rows, 0)
    drain_rows(NEAR, 0)

    def drain_returns(chunk, _):
        giving(chunk, False).wait_send()
        giving(chunk, True).wait_send()
        return 0

    lax.fori_loop(0, 14, drain_returns, 0)
    on_part(drain_pieces)
    for part in range(2):

        @pl.when(k == part)
        def _():
            for j in range(2):
                copy_weights(part, j).wait_send()
                pass_weights(part, j).wait_send()


def body(queries, keys, values, seg_ids, norm_gain, router_w, expert_ids, w_in, w_out):
    ids = expert_ids.transpose(1, 2, 3, 0).reshape(32, 2, TOK)
    vmem = pl.BlockSpec(memory_space=pltpu.VMEM)
    hbm = pl.BlockSpec(memory_space=pl.ANY)
    dma = pltpu.SemaphoreType.DMA
    bf16, f32 = jnp.bfloat16, jnp.float32
    return pl.pallas_call(
        kernel,
        out_shape=(
            jax.ShapeDtypeStruct((SEQS, TOK, 2048), bf16),
            jax.ShapeDtypeStruct((SEQS, TOK, 2048), bf16),
        ),
        in_specs=[hbm] * 3 + [vmem] * 4 + [hbm] * 2,
        out_specs=(vmem, vmem),
        scratch_shapes=[
            pltpu.VMEM((NS, HALF, HD), bf16),
            pltpu.VMEM((NS, BLK, HD), bf16),
            pltpu.VMEM((NS, BLK, HD), bf16),
            pltpu.VMEM((GROUPS, QG, HD), bf16),
            pltpu.VMEM((GROUPS, KC, HD), bf16),
            pltpu.VMEM((GROUPS, QG, KC), f32),
            pltpu.VMEM((QG, HD), f32),
            pltpu.VMEM((QG, HD), f32),
            pltpu.VMEM((QG, HD), f32),
            pltpu.VMEM((QG, HD), f32),
            pltpu.VMEM((NS, 8, TOK, HD), bf16),
            pltpu.VMEM((SEQS, NE, TOK, HD), bf16),
            pltpu.VMEM((32, TOK, SUB), bf16),
            pltpu.VMEM((NE * EPD, CAP, SUB), bf16),
            pltpu.VMEM((NE * EPD, CAP, SUB), bf16),
            pltpu.VMEM((NE * EPD, CAP, SUB), bf16),
            pltpu.VMEM((NE * EPD, CAP, SUB), bf16),
            pltpu.VMEM((2 * EPD, SUB, FFH), bf16),
            pltpu.VMEM((2 * EPD, FFH, SUB), bf16),
            pltpu.VMEM((SUB, SUB), f32),
            pltpu.VMEM((4, SUB, HD), f32),
            pltpu.VMEM((TOK, HD), bf16),
            pltpu.SemaphoreType.REGULAR,
            dma((3,)), dma((SEQS,)), dma((SEQS,)), dma((2 * SEQS,)),
            dma((NS,)), dma((NS,)), dma((NS,)), dma((SEQS,)), dma((SEQS,)),
            dma((2,)), dma(()), dma((SEQS,)), dma((NE,)), dma((NE,)), dma((NE,)), dma((NE,)),
            dma((2,)), dma((2, 2)), dma((2,)),
            dma((2,)), dma((2, 2, SEQS)), dma((2, SEQS)), dma((2, SEQS)), dma((NE,)), dma((NE,)),
        ],
        compiler_params=pltpu.CompilerParams(
            collective_id=0, has_side_effects=True, vmem_limit_bytes=56 * 1024 * 1024
        ),
        name="block",
    )(
        queries.reshape(SEQS, 2, HALF, HD), keys, values, seg_ids, ids,
        norm_gain.reshape(16, HD), router_w.T, w_in, w_out,
    )


def solution(mesh):
    return jax.shard_map(
        body,
        mesh=mesh,
        in_specs=(
            P(None, "seq", "exp"),
            P(None, "seq", "exp"),
            P(None, "seq", "exp"),
            P(),
            P(),
            P(),
            P(("seq", "exp"), None, None, None),
            P("exp", None, None),
            P("exp", None, None),
        ),
        out_specs=(P(None, ("seq", "exp"), None), P(None, ("seq", "exp"), None)),
        check_vma=False,
    )
```

```python
import functools

import jax
import jax.numpy as jnp
from jax import lax
from jax.experimental import pallas as pl
from jax.experimental.pallas import tpu as pltpu
from jax.sharding import PartitionSpec as P

HD = 128
SUB = 512
CAP = 32
NEG = -1e30
LOG2E = 1.4426950408889634

NS = 16
NE = 16
SEQS = 8
BLK = 256
HALF = 128
EPD = 4
ROWS = EPD * CAP
FFH = 1024
TOK = 16

QG = 256
KC = 512
GROUPS = 8
BIG = 2.0**100
MESH = pl.DeviceIdType.MESH


def other(seq, exp):
    return {"seq": seq, "exp": exp}


def offset_of(i):
    p = i // 2
    mag = 3 - p // 2
    return (i + 1) % 2, jnp.where(p % 2 == 0, mag, NZ - mag)


NEAR = 12
NZ = 8


def partner_to(e, i):
    dy, dz = offset_of(i)
    return (e // NZ + dy) % 2 * NZ + (e % NZ + dz) % NZ


def partner_from(e, i):
    dy, dz = offset_of(i)
    return (e // NZ + dy) % 2 * NZ + (e % NZ + NZ - dz) % NZ


def region(i):
    return EPD * i, (2 * EPD if isinstance(i, int) and i == NEAR else EPD)


def experts_of(e, chunk):
    i = chunk if not isinstance(chunk, int) or chunk < NEAR else NEAR + (chunk - NEAR) // 2
    d = partner_to(e, i)
    y, z = d // NZ, d % NZ
    home = EPD * d
    before = EPD * (y * NZ + (z + NZ - 1) % NZ)
    after = EPD * (y * NZ + (z + 1) % NZ)
    up = (i // 2) % 2 == 0 if not isinstance(chunk, int) or chunk < NEAR else chunk % 2 == 0
    ahead = (home, home + 2, after + 1, after + 3)
    behind = (home + 1, home + 3, before, before + 2)
    return tuple(jnp.where(up, f, g) for f, g in zip(ahead, behind))


def kernel(
    q_ref, k_ref, v_ref, seg_ref, ids_ref, gain_ref, rw_ref, win_hbm, wout_hbm, normed_ref, mix_ref,
    qbuf, kbuf, vbuf, qaug, kaug, sbuf, pmax, mrow, asum, aacc, obuf,
    tok, xbuf, outbuf, arrived, res, returned, win, wout, acc, cols, spare,
    ready, loc, ksend, vsend, qsend, krecv, vrecv, qrecv, kfwd, vfwd,
    wsem, osend, orecv, dsend, drecv, rsend, rrecv, wsend, wrecv, wsend2, zsend, precv, bsend, fsend, rsend2, rrecv2,
):
    s = lax.axis_index("seq")
    e = lax.axis_index("exp")
    c = s // 2
    k = s % 2
    other_core = 2 * c + 1 - k
    f32, bf16 = jnp.float32, jnp.bfloat16

    loads = (
        pltpu.make_async_copy(win_hbm, win.at[pl.ds(0, EPD)], wsem.at[0]),
        pltpu.make_async_copy(wout_hbm, wout.at[pl.ds(0, EPD)], wsem.at[1]),
    )

    barrier = pltpu.get_barrier_semaphore()

    def greet(i, _):
        pl.semaphore_signal(barrier, inc=1, device_id=other((s + i) % NS, e), device_id_type=MESH)
        pl.semaphore_signal(barrier, inc=1, device_id=other(s, (e + i) % NE), device_id_type=MESH)
        return 0

    lax.fori_loop(1, NS, greet, 0)
    pl.semaphore_wait(barrier, 2 * (NS - 1))

    def remote(src, dst, ss, rs, seq, exp):
        return pltpu.make_async_remote_copy(
            src_ref=src, dst_ref=dst, send_sem=ss, recv_sem=rs, device_id=other(seq, exp), device_id_type=MESH
        )

    def send(which, j):
        b = (c + j) % SEQS
        same = 2 * b + k
        cross = 2 * b + 1 - k
        if which == 0:
            return remote(k_ref.at[b], kbuf.at[s], ksend.at[j], krecv.at[s], same, e)
        if which == 1:
            return remote(q_ref.at[b, k], qbuf.at[s], qsend.at[j], qrecv.at[s], same, e)
        if which == 2:
            return remote(q_ref.at[b, 1 - k], qbuf.at[s], qsend.at[SEQS + j], qrecv.at[s], cross, e)
        return remote(v_ref.at[b], vbuf.at[s], vsend.at[j], vrecv.at[s], same, e)

    def start_with(*which):
        def start(j, _):
            for i in which:
                send(i, j).start()
            return 0

        lax.fori_loop(1, SEQS, start, 0)

    def copy_weights(part, j):
        src, dst = (win_hbm, win) if part == 0 else (wout_hbm, wout)
        z = (e % NZ + (1 if j == 0 else NZ - 1)) % NZ
        return remote(src.at[j], dst.at[EPD + j], wsend.at[j], wrecv.at[part, j], s, e // NZ * NZ + z)

    def pass_weights(part, j):
        buf = win if part == 0 else wout
        return remote(buf.at[EPD + j], buf.at[EPD + j], wsend2.at[j], wrecv.at[part, j], other_core, e)

    def piece_of(part, x, p):
        return (win.at[x, pl.ds(p * 64, 64)], wout.at[x, pl.ds(p * 128, 128)])[part]

    def copy_piece(part, j):
        src = (win_hbm.at[2 + j, pl.ds(c * 64, 64)], wout_hbm.at[2 + j, pl.ds(c * 128, 128)])[part]
        z = (e % NZ + (1 if j == 0 else NZ - 1)) % NZ
        return remote(src, piece_of(part, 6 + j, c), zsend.at[j], precv.at[part, j, c], s, e // NZ * NZ + z)

    def share_piece(part, j, i):
        piece = piece_of(part, 6 + j, c)
        to = other_core if isinstance(i, int) else 2 * ((c + i) % SEQS) + k
        return remote(piece, piece, bsend.at[j, i], precv.at[part, j, c], to, e)

    def pass_piece(part, j, i):
        p = (c + SEQS - i) % SEQS
        piece = piece_of(part, 6 + j, p)
        return remote(piece, piece, fsend.at[j, i], precv.at[part, j, p], other_core, e)

    def on_part(act):
        for part in range(2):
            pl.when(k == part)(functools.partial(act, part))

    def over_pieces(make, act):
        def one(i, _):
            for j in range(2):
                act(make(j, i))
            return 0

        lax.fori_loop(1, SEQS, one, 0)

    def first_weights(part):
        for j in range(2):
            copy_piece(part, j).start()
        for j in range(2):
            copy_weights(part, j).start()

    def share_weights(j, part):
        copy_piece(part, j).wait_recv()
        share_piece(part, j, 0).start()

        def one(i, _):
            share_piece(part, j, i).start()
            return 0

        lax.fori_loop(1, SEQS, one, 0)

    def pass_pieces(part):
        def go(copy):
            copy.wait_recv()
            copy.start()

        over_pieces(functools.partial(pass_piece, part), go)

    def take_pieces(part):
        def one(p, _):
            for j in range(2):
                piece = piece_of(1 - part, 6 + j, p)
                pltpu.make_async_copy(piece, piece, precv.at[1 - part, j, p]).wait()
            return 0

        lax.fori_loop(0, SEQS, one, 0)

    def drain_pieces(part):
        for j in range(2):
            copy_piece(part, j).wait_send()
            share_piece(part, j, 0).wait_send()
        over_pieces(functools.partial(share_piece, part), lambda copy: copy.wait_send())
        over_pieces(functools.partial(pass_piece, part), lambda copy: copy.wait_send())

    on_part(first_weights)
    start_with(0)
    own = (
        pltpu.make_async_copy(k_ref.at[c], kbuf.at[s], loc.at[0]),
        pltpu.make_async_copy(v_ref.at[c], vbuf.at[s], loc.at[1]),
        pltpu.make_async_copy(q_ref.at[c, k], qbuf.at[s], loc.at[2]),
    )
    near = (
        remote(k_ref.at[c], kbuf.at[s], kfwd.at[0], krecv.at[s], other_core, e),
        remote(v_ref.at[c], vbuf.at[s], vfwd.at[0], vrecv.at[s], other_core, e),
        remote(q_ref.at[c, 1 - k], qbuf.at[s], qsend.at[0], qrecv.at[s], other_core, e),
    )
    for copy in own + near:
        copy.start()
    start_with(3)
    start_with(1, 2)
    for copy in loads:
        copy.start()

    def greet_again(i, _):
        pl.semaphore_signal(ready, inc=1, device_id=other(s, (e + i) % NE), device_id_type=MESH)
        return 0

    lax.fori_loop(1, NE, greet_again, 0)

    seg = seg_ref[pl.ds(c, 1), :]
    firsts = [jnp.sum((seg < v).astype(jnp.int32)) for v in (1, 2, 3)]

    def document(pos):
        return sum((pos >= f).astype(jnp.int32) for f in firsts)

    def mark(j, _):
        key_pos = lax.broadcasted_iota(jnp.int32, (KC, HD), 0) + j * KC
        lane = lax.broadcasted_iota(jnp.int32, (KC, HD), 1)
        kaug[j] = (document(key_pos) == lane).astype(f32).astype(bf16)
        row = lax.broadcasted_iota(jnp.int32, (QG, HD), 0)
        query_pos = row + jnp.where(row >= HALF, HALF, 0) + (j * KC + k * HALF)
        lane = lax.broadcasted_iota(jnp.int32, (QG, HD), 1)
        qaug[j] = jnp.where(document(query_pos) == lane, 0.0, -BIG).astype(bf16)
        return 0

    lax.fori_loop(0, GROUPS, mark, 0)

    to_lane = (
        lax.broadcasted_iota(jnp.int32, (TOK, SUB), 0) == lax.broadcasted_iota(jnp.int32, (TOK, SUB), 1) % TOK
    ).astype(f32).astype(bf16)
    own_row = lax.broadcasted_iota(jnp.int32, (32, SUB), 0) == lax.broadcasted_iota(jnp.int32, (32, SUB), 1) // TOK
    ids = []
    for t in range(2):
        table = jnp.dot(ids_ref[:, t, :].astype(f32).astype(bf16), to_lane, preferred_element_type=f32)
        ids.append(jnp.sum(jnp.where(own_row, table, 0.0), axis=0, keepdims=True))
    experts = lax.broadcasted_iota(jnp.int32, (64, SUB), 0).astype(f32)
    before = (
        lax.broadcasted_iota(jnp.int32, (SUB, SUB), 0) < lax.broadcasted_iota(jnp.int32, (SUB, SUB), 1)
    ).astype(f32).astype(bf16)
    hot0 = (experts == ids[0]).astype(f32)
    hot1 = (experts == ids[1]).astype(f32)
    run0 = jnp.dot(hot0.astype(bf16), before, preferred_element_type=f32)
    run1 = jnp.dot(hot1.astype(bf16), before, preferred_element_type=f32)
    run1 = run1 + jnp.sum(hot0, axis=1, keepdims=True)
    slot0 = ids[0] * CAP + jnp.sum(run0 * hot0, axis=0, keepdims=True)
    slot1 = ids[1] * CAP + jnp.sum(run1 * hot1, axis=0, keepdims=True)
    lines = jnp.concatenate([slot0, slot1, *ids, jnp.zeros((124, SUB), f32)], axis=0)
    lines = jnp.transpose(lines)
    for i in range(4):
        cols[i] = jnp.broadcast_to(lines[:, i:i + 1], (SUB, HD))

    def forward(which, j):
        src = 2 * ((c + SEQS - j) % SEQS) + k
        if which == 0:
            return remote(kbuf.at[src], kbuf.at[src], kfwd.at[j], krecv.at[src], other_core, e)
        return remote(vbuf.at[src], vbuf.at[src], vfwd.at[j], vrecv.at[src], other_core, e)

    def relay_of(which):
        def relay(j, _):
            copy = forward(which, j)
            copy.wait_recv()
            copy.start()
            return 0

        lax.fori_loop(1, SEQS, relay, 0)

    def finish_of(buf, sem):
        def finish(j, _):
            src = 2 * ((c + SEQS - j) % SEQS) + 1 - k
            pltpu.make_async_copy(buf.at[src], buf.at[src], sem.at[src]).wait()
            return 0

        lax.fori_loop(0, SEQS, finish, 0)

    relay_of(0)
    relay_of(1)
    finish_of(kbuf, krecv)
    finish_of(vbuf, vrecv)
    for copy in own:
        copy.wait()
    pl.semaphore_wait(ready, NE - 1)

    scale = HD ** (-0.5) * LOG2E

    def scores_of(m, j):
        qq = jnp.concatenate([qbuf[pl.ds(2 * m, 2)].reshape(QG, HD), qaug[m]], axis=1)
        kk = jnp.concatenate([kbuf[pl.ds(2 * j, 2)].reshape(KC, HD), kaug[j]], axis=1)
        return lax.dot_general(qq, kk, (((1,), (1,)), ((), ())), preferred_element_type=f32)

    def tiles(x, op):
        out = x[:, 0:HD]
        for i in range(1, KC // HD):
            out = op(out, x[:, i * HD:(i + 1) * HD])
        return out

    def first_pass(m, j, count):
        highest = pmax[...]
        for i in range(count):
            scores = scores_of(m, j + i)
            sbuf[j + i] = scores
            highest = jnp.maximum(highest, tiles(scores, jnp.maximum))
        pmax[...] = highest

    def second_pass(m, j, count):
        top = jnp.concatenate([mrow[...]] * (KC // HD), axis=1)
        total = asum[...]
        out = aacc[...]
        for i in range(count):
            weights = jnp.exp2((sbuf[j + i] - top) * scale)
            total = total + tiles(weights, jnp.add)
            vv = vbuf[pl.ds(2 * (j + i), 2)].reshape(KC, HD)
            out = out + jnp.dot(weights.astype(bf16), vv, preferred_element_type=f32)
        asum[...] = total
        aacc[...] = out

    def attend(t, _):
        m = (c + GROUPS - t) % GROUPS
        for i in range(2):
            src = 2 * m + i

            @pl.when(src != s)
            def _():
                pltpu.make_async_copy(qbuf.at[src], qbuf.at[src], qrecv.at[src]).wait()

        pmax[...] = jnp.full((QG, HD), -BIG, f32)
        asum[...] = jnp.zeros((QG, HD), f32)
        aacc[...] = jnp.zeros((QG, HD), f32)

        def score(j, _):
            first_pass(m, 2 * j, 2)
            return 0

        lax.fori_loop(0, m // 2, score, 0)

        @pl.when(m % 2 == 1)
        def _():
            first_pass(m, m - 1, 1)

        scores = scores_of(m, m)
        row = lax.broadcasted_iota(jnp.int32, (QG, KC), 0)
        row = row + jnp.where(row >= HALF, HALF, 0) + k * HALF
        scores = jnp.where(lax.broadcasted_iota(jnp.int32, (QG, KC), 1) <= row, scores, -BIG)
        sbuf[m] = scores
        highest = jnp.maximum(pmax[...], tiles(scores, jnp.maximum))
        mrow[...] = jnp.broadcast_to(jnp.max(highest, axis=-1, keepdims=True), (QG, HD))

        def step(j, _):
            second_pass(m, 2 * j, 2)
            return 0

        lax.fori_loop(0, (m + 1) // 2, step, 0)

        @pl.when(m % 2 == 0)
        def _():
            second_pass(m, m, 1)

        total = jnp.sum(asum[...], axis=-1, keepdims=True)
        obuf[pl.ds(2 * m, 2)] = (aacc[...] / total).astype(bf16).reshape(2, 8, TOK, HD)

        for i in range(16):
            sp = 2 * m + i // 8
            ei = (e + i) % 8
            copy = remote(obuf.at[sp, ei], tok.at[c, e], osend, orecv.at[c], sp, k * 8 + ei)
            if i % 8:
                copy.start()
                continue
            mine = (sp == s) & (k == e // 8)
            pl.when(jnp.logical_not(mine))(copy.start)

            @pl.when(mine)
            def _():
                pltpu.make_async_copy(obuf.at[sp, ei], tok.at[c, e], orecv.at[c]).start()
                pltpu.make_async_copy(obuf.at[sp, ei], spare, osend).start()

        return 0

    lax.fori_loop(0, GROUPS, attend, 0)

    on_part(functools.partial(share_weights, 0))

    for part in range(2):

        @pl.when(k == part)
        def _():
            for j in range(2):
                copy = pass_weights(part, j)
                copy.wait_recv()
                copy.start()

    gain = gain_ref[...]

    def norm(b, _):
        pltpu.make_async_copy(tok.at[b], tok.at[b], orecv.at[b]).wait()
        v = tok[b].astype(f32)
        square = jnp.sum(jnp.sum(v * v, axis=0), axis=-1, keepdims=True)
        spread = jnp.sqrt(square * (1.0 / 2048.0) + 1e-6)
        n = (v / spread[None] * gain[:, None, :]).astype(bf16)
        for h in range(16):
            normed_ref[b, :, h * HD:(h + 1) * HD] = n[h]
            xbuf[b * 4 + h // 4, :, (h % 4) * HD:(h % 4 + 1) * HD] = n[h]
        return 0

    lax.fori_loop(0, SEQS, norm, 0)

    on_part(functools.partial(share_weights, 1))

    def rows_at(buf, i):
        first, count = region(i)
        return buf.at[pl.ds(first, count)]

    def sending(i):
        return remote(rows_at(outbuf, i), rows_at(arrived, i), dsend.at[i], drecv.at[i], s, partner_to(e, i))

    slot_line = lax.broadcasted_iota(jnp.int32, (CAP, SUB), 0)

    def gathered(chunk):
        slot = jnp.concatenate([slot_line + x * CAP for x in experts_of(e, chunk)], axis=0).astype(f32)
        chosen = ((slot == slot0) | (slot == slot1)).astype(f32).astype(bf16)
        rows = jnp.dot(chosen, xbuf[...].reshape(SUB, SUB), preferred_element_type=f32)
        return rows.astype(bf16).reshape(EPD, CAP, SUB)

    def dispatch(i, _):
        outbuf[pl.ds(EPD * i, EPD)] = gathered(i)
        sending(i).start()
        return 0

    lax.fori_loop(0, NEAR, dispatch, 0)
    outbuf[48:52] = gathered(12)
    outbuf[52:56] = gathered(13)
    sending(NEAR).start()
    arrived[56:60] = gathered(14)
    arrived[60:64] = gathered(15)

    logits = lax.dot_general(
        xbuf[...].reshape(SUB, SUB), rw_ref[...], (((1,), (1,)), ((), ())), preferred_element_type=f32
    )
    lanes64 = lax.broadcasted_iota(jnp.int32, (SUB, 64), 1).astype(f32)
    picked = [
        jnp.sum(jnp.where(lanes64 == cols[2 + t][:, 0:64], logits, 0.0), axis=1, keepdims=True) for t in range(2)
    ]
    sig0 = 1.0 / (1.0 + jnp.exp(-picked[0]))
    sig1 = 1.0 / (1.0 + jnp.exp(-picked[1]))
    cols[2] = jnp.broadcast_to(sig0 / (sig0 + sig1), (SUB, HD))
    cols[3] = jnp.broadcast_to(sig1 / (sig0 + sig1), (SUB, HD))
    acc[...] = jnp.zeros((SUB, SUB), f32)

    for copy in loads:
        copy.wait()
    for part in range(2):

        @pl.when(k != part)
        def _():
            for j in range(2):
                buf = (win if part == 0 else wout).at[EPD + j]
                pltpu.make_async_copy(buf, buf, wrecv.at[part, j]).wait()

    def giving(chunk, late):
        i = jnp.minimum(chunk, NEAR)
        first, count = (EPD * chunk + 3, 1) if late else (EPD * chunk, 3)
        return remote(
            res.at[pl.ds(first, count)], returned.at[pl.ds(first, count)],
            (rsend2 if late else rsend).at[chunk], (rrecv2 if late else rrecv).at[chunk], s, partner_from(e, i),
        )

    def run_expert(chunks, xp, w):
        a = jnp.concatenate([arrived[EPD * at + xp] for at in chunks], axis=0)
        u = jnp.dot(a, win[w], preferred_element_type=f32)
        hid = 0.5 * u * (1.0 + jnp.tanh(0.7978845608028654 * (u + 0.044715 * (u * u * u))))
        y = jnp.dot(hid.astype(bf16), wout[w], preferred_element_type=f32).astype(bf16)
        for j in range(4):
            res[EPD * chunks[j] + xp] = y[j * CAP:(j + 1) * CAP]

    plan = (
        ((0, 1, 4, 5), (0, 1, 4, 5), True),
        ((2, 3, 6, 7), (2, 3, 6, 7), False),
        ((8, 9, 12), (8, 9, 12, 14), True),
        ((10, 11), (10, 11, 13, 15), False),
    )
    for needed, chunks, up in plan:
        for i in needed:
            part = rows_at(arrived, i)
            pltpu.make_async_copy(part, part, drecv.at[i]).wait()

        def early(xp, _):
            late = jnp.where(xp >= 2, 1, 0)
            run_expert(chunks, xp, 2 * xp + late if up else 2 * xp + 1 - late)
            return 0

        lax.fori_loop(0, 3, early, 0)
        for chunk in chunks:
            if chunk < 14:
                giving(chunk, False).start()

    on_part(pass_pieces)
    on_part(take_pieces)
    for _, chunks, up in plan:
        run_expert(chunks, 3, 7 if up else 6)
        for chunk in chunks:
            if chunk < 14:
                giving(chunk, True).start()
    returned[56:64] = res[56:64]

    lane = lax.broadcasted_iota(jnp.int32, (SUB, HD), 1)

    def table_of(chunk):
        x = experts_of(e, chunk)
        part = lane // CAP
        slot = jnp.where(part < 2, jnp.where(part == 0, x[0], x[1]), jnp.where(part == 2, x[2], x[3]))
        slot = (slot * CAP + lane % CAP).astype(f32)
        return jnp.where(slot == cols[0], cols[2], 0.0) + jnp.where(slot == cols[1], cols[3], 0.0)

    def add_rows(tables, parts):
        table = jnp.concatenate(tables, axis=1)
        rows = jnp.concatenate(parts, axis=0)
        high = table.astype(bf16)
        low = (table - high.astype(f32)).astype(bf16)
        acc[...] += jnp.dot(high, rows, preferred_element_type=f32) + jnp.dot(low, rows, preferred_element_type=f32)

    def chunk_rows(chunk):
        return returned[pl.ds(EPD * chunk, EPD)].reshape(ROWS, SUB)

    def wait_rows(chunk):
        for first, count, sem in ((EPD * chunk, 3, rrecv), (EPD * chunk + 3, 1, rrecv2)):
            part = returned.at[pl.ds(first, count)]
            pltpu.make_async_copy(part, part, sem.at[chunk]).wait()

    add_rows([table_of(14), table_of(15)], [chunk_rows(14), chunk_rows(15)])

    def combine(a, b):
        wait_rows(a)
        wait_rows(b)
        add_rows([table_of(a), table_of(b)], [chunk_rows(a), chunk_rows(b)])

    for first in (0, 4, 2, 6, 8):
        combine(first, first + 1)
    combine(10, 11)
    combine(12, 13)
    for b in range(SEQS):
        for g in range(4):
            mix_ref[b, :, g * SUB:(g + 1) * SUB] = acc[(b * 4 + g) * TOK:(b * 4 + g + 1) * TOK].astype(bf16)

    pltpu.make_async_copy(obuf, obuf, osend).wait()

    def drain(j, _):
        for i in range(4):
            send(i, j).wait_send()
        for i in range(2):
            forward(i, j).wait_send()
        return 0

    lax.fori_loop(1, SEQS, drain, 0)
    for copy in near:
        copy.wait_send()

    def drain_rows(i, _):
        sending(i).wait_send()
        return 0

    lax.fori_loop(0, NEAR, drain_rows, 0)
    drain_rows(NEAR, 0)

    def drain_returns(chunk, _):
        giving(chunk, False).wait_send()
        giving(chunk, True).wait_send()
        return 0

    lax.fori_loop(0, 14, drain_returns, 0)
    on_part(drain_pieces)
    for part in range(2):

        @pl.when(k == part)
        def _():
            for j in range(2):
                copy_weights(part, j).wait_send()
                pass_weights(part, j).wait_send()


def hand_on(normed_ref, mix_ref, normed_out, mix_out):
    normed_out[...] = normed_ref[...]
    mix_out[...] = mix_ref[...]


def body(queries, keys, values, seg_ids, norm_gain, router_w, expert_ids, w_in, w_out):
    ids = expert_ids.transpose(1, 2, 3, 0).reshape(32, 2, TOK)
    vmem = pl.BlockSpec(memory_space=pltpu.VMEM)
    hbm = pl.BlockSpec(memory_space=pl.ANY)
    dma = pltpu.SemaphoreType.DMA
    bf16, f32 = jnp.bfloat16, jnp.float32
    results = pl.pallas_call(
        kernel,
        out_shape=(
            jax.ShapeDtypeStruct((SEQS, TOK, 2048), bf16),
            jax.ShapeDtypeStruct((SEQS, TOK, 2048), bf16),
        ),
        in_specs=[hbm] * 3 + [vmem] * 4 + [hbm] * 2,
        out_specs=(vmem, vmem),
        scratch_shapes=[
            pltpu.VMEM((NS, HALF, HD), bf16),
            pltpu.VMEM((NS, BLK, HD), bf16),
            pltpu.VMEM((NS, BLK, HD), bf16),
            pltpu.VMEM((GROUPS, QG, HD), bf16),
            pltpu.VMEM((GROUPS, KC, HD), bf16),
            pltpu.VMEM((GROUPS, QG, KC), f32),
            pltpu.VMEM((QG, HD), f32),
            pltpu.VMEM((QG, HD), f32),
            pltpu.VMEM((QG, HD), f32),
            pltpu.VMEM((QG, HD), f32),
            pltpu.VMEM((NS, 8, TOK, HD), bf16),
            pltpu.VMEM((SEQS, NE, TOK, HD), bf16),
            pltpu.VMEM((32, TOK, SUB), bf16),
            pltpu.VMEM((NE * EPD, CAP, SUB), bf16),
            pltpu.VMEM((NE * EPD, CAP, SUB), bf16),
            pltpu.VMEM((NE * EPD, CAP, SUB), bf16),
            pltpu.VMEM((NE * EPD, CAP, SUB), bf16),
            pltpu.VMEM((2 * EPD, SUB, FFH), bf16),
            pltpu.VMEM((2 * EPD, FFH, SUB), bf16),
            pltpu.VMEM((SUB, SUB), f32),
            pltpu.VMEM((4, SUB, HD), f32),
            pltpu.VMEM((TOK, HD), bf16),
            pltpu.SemaphoreType.REGULAR,
            dma((3,)), dma((SEQS,)), dma((SEQS,)), dma((2 * SEQS,)),
            dma((NS,)), dma((NS,)), dma((NS,)), dma((SEQS,)), dma((SEQS,)),
            dma((2,)), dma(()), dma((SEQS,)), dma((NE,)), dma((NE,)), dma((NE,)), dma((NE,)),
            dma((2,)), dma((2, 2)), dma((2,)),
            dma((2,)), dma((2, 2, SEQS)), dma((2, SEQS)), dma((2, SEQS)), dma((NE,)), dma((NE,)),
        ],
        compiler_params=pltpu.CompilerParams(
            collective_id=0, has_side_effects=True, vmem_limit_bytes=56 * 1024 * 1024
        ),
        name="block",
    )(
        queries.reshape(SEQS, 2, HALF, HD), keys, values, seg_ids, ids,
        norm_gain.reshape(16, HD), router_w.T, w_in, w_out,
    )
    tokens = pl.BlockSpec((2, TOK, 2048), lambda i: (i, 0, 0))
    return pl.pallas_call(
        hand_on,
        out_shape=(jax.ShapeDtypeStruct((SEQS, TOK, 2048), bf16),) * 2,
        grid=(SEQS // 2,),
        in_specs=[tokens, tokens],
        out_specs=(tokens, tokens),
        name="hand_on",
    )(*results)


def solution(mesh):
    return jax.shard_map(
        body,
        mesh=mesh,
        in_specs=(
            P(None, "seq", "exp"),
            P(None, "seq", "exp"),
            P(None, "seq", "exp"),
            P(),
            P(),
            P(),
            P(("seq", "exp"), None, None, None),
            P("exp", None, None),
            P("exp", None, None),
        ),
        out_specs=(P(None, ("seq", "exp"), None), P(None, ("seq", "exp"), None)),
        check_vma=False,
    )
```
